256 devices in a mesh: gx: 4 (over x), gy: 64 (over z, y, core).
Axes of the slice: x: 4, y: 4, z: 8, core: 2. Of those that a mesh axis runs over, the one named last changes fastest.
Arguments:
- features: bfloat16 [262144, 768], P(('gx', 'gy')), may hold values from -6 to 6
- seed_rows: int32 [16384], P(('gx', 'gy')), may hold values from 0 to 1023
- hop1_ids: int32 [16384, 5], P(('gx', 'gy')), may hold values from 0 to 262143, as said below
- hop2_ids: int32 [16384, 5, 5], P(('gx', 'gy')), may hold values from 0 to 262143, as said below
- w_self: bfloat16 [768, 1024], replicated, may hold values from -0.21875 to 0.21875
- w_neigh: bfloat16 [768, 1024], replicated, may hold values from -0.21875 to 0.21875
- bias: float32 [1024], replicated, may hold values from -3 to 3
- cotangent: bfloat16 [16384, 1024], P(('gx', 'gy')), may hold values from -6 to 6
Outputs:
- embedded: bfloat16 [16384, 1024], P(('gx', 'gy'))
- grad_self: float32 [768, 1024], P(None, ('gx', 'gy'))
- grad_neigh: float32 [768, 1024], P(None, ('gx', 'gy'))
- grad_bias: float32 [1024], P(('gx', 'gy'))
The draws below stay inside these ranges and needn't reach their ends.
Inputs may be any that keep to these rules, and one draw needn't show every extreme that they name: `hop1_ids`: row i belongs to device i // 1024 (device index gx * 64 + gy). The 320 entries of one device name at most 2 rows of any one owner, repeats counted; in every draw one owner receives exactly 2 from every device. `hop2_ids`: row i belongs to device i // 1024. The 1600 entries of one device name at most 9 rows of any one owner, repeats counted; in every draw one owner receives exactly 9 from every device.
All inputs are finite; a program needn't handle non-finite values.
Results may differ from the reference program's by a relative error of at most 0.025.
The reference program's roundings to bfloat16 on the way (of `x_seed`, `x_near`, `pooled_far`, `hidden_near`, `pooled_near`, `hidden_seed` and `spread`) count: a program that leaves them out, or rounds other values in their place, can miss the bound.
Values may be sent and summed in bfloat16 or wider, within the bound.
No kernel may reach another device: no remote copies, remote signals or barrier semaphores. Data moves between devices by JAX's collectives and lax.ppermute only.
A program may use at most 64 MiB of HBM per device.

```python
import jax
import jax.numpy as jnp
from jax import lax

F = 768
H = 1024
SEEDS = 64
ROWS_DEV = 1024
K1 = 5
K2 = 5
NODES = 262144
SEEDS_ALL = 16384
CAP1 = 2
CAP2 = 9
N_GX = 4
N_GY = 64


def plan_owners(key, item_count, capacity):
    devices = N_GX * N_GY
    hot_owner = jax.random.randint(jax.random.fold_in(key, 7), (), 0, devices)
    device_keys = jax.random.split(jax.random.fold_in(key, 11), devices)

    def per_device(device_key):
        key_perm, key_shuffle, key_rows = jax.random.split(device_key, 3)
        shuffled = jax.random.permutation(key_perm, devices * capacity)
        priority = jnp.where(shuffled // capacity == hot_owner, 0, 1 + jnp.arange(devices * capacity))
        chosen = shuffled[jnp.argsort(priority, stable=True)][:item_count]
        chosen = chosen[jax.random.permutation(key_shuffle, item_count)]
        owners = chosen // capacity
        row_ids = jax.random.randint(key_rows, (item_count,), 0, ROWS_DEV)
        return (owners * ROWS_DEV + row_ids).astype(jnp.int32)
    return jax.vmap(per_device)(device_keys)


def draw_hop1_ids(key, part):
    picked = plan_owners(jax.random.fold_in(key, 101), SEEDS * K1, CAP1)
    return picked.reshape(SEEDS_ALL, K1).astype(jnp.int32)


def draw_hop2_ids(key, part):
    picked = plan_owners(jax.random.fold_in(key, 202), SEEDS * K1 * K2, CAP2)
    return picked.reshape(SEEDS_ALL, K1, K2).astype(jnp.int32)


def place_ends(values, stream_key, smallest, largest):
    longest = values.shape.index(max(values.shape))
    spots = []
    for shift in (0, 1):
        where = [jax.random.randint(jax.random.fold_in(stream_key, axis), (), 0, length) for axis, length in enumerate(values.shape)]
        where[longest] = (where[longest] + shift) % values.shape[longest]
        spots.append(tuple(where))
    return values.at[spots[0]].set(smallest).at[spots[1]].set(largest)


def steps_of(key, shape, shards, least, high):
    factor_of, own = 1.0, jax.random.fold_in(key, 6)
    for dim, blocks in shards:
        steps = jnp.exp(jax.random.uniform(jax.random.fold_in(own, dim), (blocks,), jnp.float32, least / len(shards), high / len(shards)))
        factor_of = factor_of * jnp.repeat(steps, shape[dim] // blocks).reshape([-1 if axis == dim else 1 for axis in range(len(shape))])
    return factor_of


def centred(rng, extent, width, most, cuts=(), held_as=jnp.bfloat16):
    factor_of = steps_of(rng, extent, cuts, -0.22, 0.18) if cuts else 1.0
    drawn = jax.random.normal(rng, extent, jnp.float32) * width * factor_of
    return jnp.minimum(jnp.maximum(drawn, -most), most).astype(held_as)


def setup_inputs(seed: int = 0) -> dict:
    seeds = jax.random.split(jax.random.key(seed), 9)
    return {
        "features": centred(seeds[0], (NODES, F), 1.0, 6.0, ((0, 256),)),
        "seed_rows": place_ends(jax.random.randint(seeds[1], (SEEDS_ALL,), 0, ROWS_DEV), jax.random.fold_in(seeds[1], 1), 0, ROWS_DEV - 1).astype(jnp.int32),
        "hop1_ids": draw_hop1_ids(jax.random.fold_in(seeds[8], 71), 0),
        "hop2_ids": draw_hop2_ids(jax.random.fold_in(seeds[8], 71), 0),
        "w_self": centred(seeds[4], (F, H), F ** -0.5, 0.21875),
        "w_neigh": centred(seeds[5], (F, H), F ** -0.5, 0.21875),
        "bias": centred(seeds[6], (H,), 0.5, 3.0, (), jnp.float32),
        "cotangent": centred(seeds[7], (SEEDS_ALL, H), 1.0, 6.0, ((0, 256),)),
    }


def contract_rows(left, right):
    return lax.dot_general(left.astype(jnp.float32), right.astype(jnp.float32), (((0,), (0,)), ((), ())))


def reference(features, seed_rows, hop1_ids, hop2_ids, w_self, w_neigh, bias, cotangent):
    devices = N_GX * N_GY
    offsets = jnp.arange(devices, dtype=jnp.int32) * ROWS_DEV
    seed_ids = seed_rows.reshape(devices, SEEDS).astype(jnp.int32) + offsets[:, None]
    near_ids = hop1_ids.reshape(devices, SEEDS * K1)
    far_ids = hop2_ids.reshape(devices, SEEDS * K1 * K2)
    cot_parts = cotangent.reshape(devices, SEEDS, H)

    def visit_device(totals, inputs):
        grad_self, grad_neigh, grad_bias = totals
        seed_id, near_id, far_id, cot_part = inputs
        x_seed = features[seed_id]
        x_near = features[near_id]
        far_rows = features[far_id].astype(jnp.float32).reshape(SEEDS * K1, K2, F)
        pooled_far = (jnp.sum(far_rows, axis=1) / K2).astype(jnp.bfloat16)
        pre_near = (jnp.dot(x_near, w_self, preferred_element_type=jnp.float32)
                    + jnp.dot(pooled_far, w_neigh, preferred_element_type=jnp.float32) + bias)
        hidden_near = jnp.maximum(pre_near, 0.0).astype(jnp.bfloat16)
        pooled_near = (jnp.sum(x_near.astype(jnp.float32).reshape(SEEDS, K1, F), axis=1) / K1).astype(jnp.bfloat16)
        pre_seed = (jnp.dot(x_seed, w_self, preferred_element_type=jnp.float32)
                    + jnp.dot(pooled_near, w_neigh, preferred_element_type=jnp.float32) + bias)
        hidden_seed = jnp.maximum(pre_seed, 0.0).astype(jnp.bfloat16)
        summed = hidden_seed.astype(jnp.float32) + jnp.sum(hidden_near.astype(jnp.float32).reshape(SEEDS, K1, H), axis=1)
        embedded = (summed / (1 + K1)).astype(jnp.bfloat16)
        spread = (cot_part.astype(jnp.float32) / (1 + K1)).astype(jnp.bfloat16)
        zero_value = jnp.zeros((), jnp.bfloat16)
        delta_seed = jnp.where(pre_seed > 0, spread, zero_value)
        delta_near = jnp.where(pre_near > 0, jnp.repeat(spread, K1, axis=0), zero_value)
        grad_self = grad_self + contract_rows(x_seed, delta_seed) + contract_rows(x_near, delta_near)
        grad_neigh = grad_neigh + contract_rows(pooled_near, delta_seed) + contract_rows(pooled_far, delta_near)
        grad_bias = (grad_bias + jnp.sum(delta_seed.astype(jnp.float32), axis=0)
                     + jnp.sum(delta_near.astype(jnp.float32), axis=0))
        return (grad_self, grad_neigh, grad_bias), embedded

    starting = (jnp.zeros((F, H), jnp.float32), jnp.zeros((F, H), jnp.float32), jnp.zeros((H,), jnp.float32))
    totals, embedded = lax.scan(visit_device, starting, (seed_ids, near_ids, far_ids, cot_parts))
    return embedded.reshape(SEEDS_ALL, H), totals[0], totals[1], totals[2]
```

```python
import functools

import jax
import jax.numpy as jnp
import numpy as np
from jax import lax
from jax.experimental import pallas as pl
from jax.experimental.pallas import tpu as pltpu
from jax.sharding import Mesh
from jax.sharding import PartitionSpec as P

GX_GY = ("gx", "gy_0", "gy_1", "gy_2")
FAR_CAP = 9
NEAR_CAP = 2
SLOTS = 16
MAIN = 8
EXTRA = 4
PLAN_BLOCK = 256
BF16 = jnp.bfloat16
F32 = jnp.float32
INTERPRET = False

NN = (((1,), (0,)), ((), ()))
NT = (((1,), (1,)), ((), ()))


def dot(left, right, dims=NN):
    return lax.dot_general(left, right, dims, preferred_element_type=F32)


def round_up(value, step):
    return -(-value // step) * step


def plan_kernel(devices, row_bits, far_blocks, ids_ref, base_ref, group_ref, request_ref, groups_ref):
    lanes = ids_ref.shape[1]
    block = PLAN_BLOCK
    upper = (
        lax.broadcasted_iota(jnp.int32, (block, block), 0) < lax.broadcasted_iota(jnp.int32, (block, block), 1)
    ).astype(F32).astype(BF16)
    owner_at = lax.broadcasted_iota(jnp.int32, (devices, block), 0)
    slot_at = lax.broadcasted_iota(jnp.int32, (SLOTS, block), 0)
    carry = jnp.zeros((devices, 1), F32)
    request = jnp.zeros((devices, SLOTS), F32)
    groups = jnp.zeros((devices, SLOTS), F32)
    for at in range(lanes // block):
        here = slice(at * block, (at + 1) * block)
        ids = ids_ref[:, here]
        if at == far_blocks:
            carry = jnp.zeros((devices, 1), F32)
        match = (owner_at == lax.shift_right_arithmetic(ids, row_bits)).astype(F32)
        match_low = match.astype(BF16)
        before = dot(match_low, upper) + carry
        carry = carry + jnp.sum(match, axis=1, keepdims=True)
        rank = jnp.sum(match * before, axis=0, keepdims=True)
        slot = rank.astype(jnp.int32) + base_ref[:, here]
        placed = (slot_at == slot).astype(F32)
        local = ids & ((1 << row_bits) - 1)
        low = local & 31
        group = group_ref[:, here]
        group_low = group & 31
        request = request + dot(match_low, (placed * (local - low).astype(F32)).astype(BF16), NT)
        request = request + dot(match_low, (placed * low.astype(F32)).astype(BF16), NT)
        groups = groups + dot(match_low, (placed * (group - group_low).astype(F32)).astype(BF16), NT)
        groups = groups + dot(match_low, (placed * group_low.astype(F32)).astype(BF16), NT)
    request_ref[...] = request.astype(jnp.int32)
    groups_ref[...] = groups.astype(jnp.int32) - 1


def plan(near_ids, far_ids, devices, row_bits):
    seeds, fan_one = near_ids.shape
    fan_two = far_ids.shape[2]
    far_total = seeds * fan_one * fan_two
    near_total = seeds * fan_one
    far_lanes = round_up(far_total, PLAN_BLOCK)
    near_lanes = round_up(near_total, PLAN_BLOCK)
    ids = jnp.concatenate(
        [
            jnp.pad(far_ids.reshape(1, -1), ((0, 0), (0, far_lanes - far_total)), constant_values=-1),
            jnp.pad(near_ids.reshape(1, -1), ((0, 0), (0, near_lanes - near_total)), constant_values=-1),
        ],
        axis=1,
    )
    lanes = far_lanes + near_lanes
    base = np.zeros((1, lanes), np.int32)
    base[:, far_lanes:] = FAR_CAP
    group = np.zeros((1, lanes), np.int32)
    far_at = np.arange(far_total)
    group[0, :far_total] = (far_at // fan_two) % fan_one * seeds + far_at // (fan_one * fan_two) + 1
    near_at = np.arange(near_total)
    group[0, far_lanes : far_lanes + near_total] = near_at % fan_one * seeds + near_at // fan_one + 1
    out = jax.ShapeDtypeStruct((devices, SLOTS), jnp.int32)
    return pl.pallas_call(
        lambda *refs: plan_kernel(devices, row_bits, far_lanes // PLAN_BLOCK, *refs),
        out_shape=(out, out),
        name="plan",
        interpret=INTERPRET,
    )(ids, jnp.asarray(base), jnp.asarray(group))


def serve_kernel(asked_ref, features_ref, out_ref):
    peers = asked_ref.shape[0]
    rows_dev, width = features_ref.shape
    half = width // 2
    asked = jnp.broadcast_to(asked_ref[...].astype(F32), (peers, MAIN, SLOTS))
    lane = lax.broadcasted_iota(jnp.int32, (peers, MAIN, SLOTS), 2)
    place = lax.broadcasted_iota(jnp.int32, (peers, MAIN, SLOTS), 1)
    row_at = lax.broadcasted_iota(jnp.int32, (peers, MAIN, rows_dev), 2).astype(F32)

    def rows_of(slot):
        chosen = jnp.sum(jnp.where(lane == slot, asked, 0.0), axis=2, keepdims=True)
        picks = (row_at == chosen).astype(F32).reshape(peers * MAIN, rows_dev).astype(BF16)
        return dot(picks, features_ref[...])

    out_ref[:, :width] = rows_of(place).astype(BF16)
    extra = rows_of(MAIN + place % EXTRA)
    part = lax.broadcasted_iota(jnp.int32, (peers * MAIN, half), 0) % MAIN
    out_ref[:, width:] = jnp.where(part < EXTRA, extra[:, :half], extra[:, half:]).astype(BF16)


def serve(asked, features, steps=8):
    devices = asked.shape[0]
    rows_dev, width = features.shape
    peers = devices // steps
    payload = width + width // 2
    return pl.pallas_call(
        serve_kernel,
        grid=(steps,),
        in_specs=[
            pl.BlockSpec((peers, 1, SLOTS), lambda i: (i, 0, 0)),
            pl.BlockSpec((rows_dev, width), lambda i: (0, 0)),
        ],
        out_specs=pl.BlockSpec((peers * MAIN, payload), lambda i: (i, 0)),
        out_shape=jax.ShapeDtypeStruct((devices * MAIN, payload), BF16),
        name="serve",
        interpret=INTERPRET,
    )(asked, features)


def layer_kernel(
    take_steps, fan_one, fan_two, rows_ref, main_ref, far_ref, near_ref, seed_ref, self_ref, neigh_ref,
    bias_ref, spread_ref, embedded_ref, grad_ref, far_acc, near_acc, own, pooled,
):
    step = pl.program_id(0)
    seeds, width = seed_ref.shape
    half = width // 2
    near_total = near_acc.shape[0]

    @pl.when(step == 0)
    def _():
        far_acc[...] = jnp.zeros_like(far_acc)
        near_acc[...] = jnp.zeros_like(near_acc)

    @pl.when(step < take_steps)
    def _():
        lanes = rows_ref.shape[0]
        group_at = lax.broadcasted_iota(jnp.int32, (near_total, lanes), 0)
        first = lax.broadcasted_iota(jnp.int32, (1, lanes), 1) % MAIN < EXTRA

        def picks(groups):
            return (group_at == groups).astype(F32).astype(BF16)

        extra = rows_ref[:, width:]
        far = far_ref[...]
        near = near_ref[...]
        far_acc[...] += dot(picks(main_ref[...]), rows_ref[:, :width])
        far_acc[:, :half] += dot(picks(jnp.where(first, far, -1)), extra)
        far_acc[:, half:] += dot(picks(jnp.where(first, -1, far)), extra)
        near_acc[:, :half] += dot(picks(jnp.where(first, near, -1)), extra)
        near_acc[:, half:] += dot(picks(jnp.where(first, -1, near)), extra)

    @pl.when(step == take_steps - 1)
    def _():
        own[:near_total] = near_acc[...].astype(BF16)
        own[near_total:] = seed_ref[...]
        pooled[:near_total] = (far_acc[...] / fan_two).astype(BF16)
        summed = near_acc[:seeds]
        for k in range(1, fan_one):
            summed = summed + near_acc[k * seeds : (k + 1) * seeds]
        pooled[near_total:] = (summed / fan_one).astype(BF16)

    @pl.when(step >= take_steps)
    def _():
        pre = dot(own[...], self_ref[...]) + dot(pooled[...], neigh_ref[...]) + bias_ref[...]
        hidden = jnp.maximum(pre, 0.0).astype(BF16).astype(F32)
        summed = hidden[near_total:]
        for k in range(fan_one):
            summed = summed + hidden[k * seeds : (k + 1) * seeds]
        embedded_ref[...] = (summed / (1 + fan_one)).astype(BF16)
        spread = spread_ref[...].astype(F32)
        delta = jnp.where(pre > 0, jnp.concatenate([spread] * (1 + fan_one), axis=0), 0.0)
        turned = delta.T.astype(BF16)
        grad_ref[:, :width] = dot(turned, own[...]).astype(BF16)
        grad_ref[:, width : 2 * width] = dot(turned, pooled[...]).astype(BF16)
        ones = (lax.broadcasted_iota(jnp.int32, (delta.shape[0], 128), 1) == 0).astype(F32).astype(BF16)
        grad_ref[:, 2 * width :] = dot(turned, ones).astype(BF16)


def layer(rows, main, far, near, seed_x, w_self, w_neigh, bias, spread, fan_one, fan_two, take_steps=8, hidden_steps=4):
    total, payload = rows.shape
    seeds, width = seed_x.shape
    hidden = w_self.shape[1]
    lanes = total // take_steps
    part = hidden // hidden_steps
    near_total = seeds * fan_one
    steps = take_steps + hidden_steps
    early = lambda i: jnp.minimum(i, take_steps - 1)
    late = lambda i: jnp.maximum(i - take_steps, 0)
    groups = pl.BlockSpec((1, lanes), lambda i: (0, early(i)))
    weights = pl.BlockSpec((width, part), lambda i: (0, late(i)))
    return pl.pallas_call(
        functools.partial(layer_kernel, take_steps, fan_one, fan_two),
        grid=(steps,),
        in_specs=[
            pl.BlockSpec((lanes, payload), lambda i: (early(i), 0)),
            groups,
            groups,
            groups,
            pl.BlockSpec((seeds, width), lambda i: (0, 0)),
            weights,
            weights,
            pl.BlockSpec((1, part), lambda i: (0, late(i))),
            pl.BlockSpec((seeds, part), lambda i: (0, late(i))),
        ],
        out_specs=(
            pl.BlockSpec((seeds, part), lambda i: (0, late(i))),
            pl.BlockSpec((part, 2 * width + 128), lambda i: (late(i), 0)),
        ),
        out_shape=(
            jax.ShapeDtypeStruct((seeds, hidden), BF16),
            jax.ShapeDtypeStruct((hidden, 2 * width + 128), BF16),
        ),
        scratch_shapes=[
            pltpu.VMEM((near_total, width), F32),
            pltpu.VMEM((near_total, width), F32),
            pltpu.VMEM((near_total + seeds, width), BF16),
            pltpu.VMEM((near_total + seeds, width), BF16),
        ],
        name="layer",
        interpret=INTERPRET,
    )(rows, main, far, near, seed_x, w_self, w_neigh, bias, spread)


def exchange(pieces, axes):
    return lax.all_to_all(pieces, axes, split_axis=0, concat_axis=0, tiled=True)


def slot_lanes(groups, devices):
    main = groups[:, :MAIN].reshape(1, -1)
    extra = groups[:, MAIN : MAIN + EXTRA]
    at = jnp.arange(EXTRA, dtype=jnp.int32)[None, :]
    far = jnp.where(at < FAR_CAP - MAIN, extra, -1)
    near = jnp.where(at >= FAR_CAP - MAIN, extra, -1)
    twice = lambda x: jnp.concatenate([x, x], axis=1).reshape(1, -1)
    return main, twice(far), twice(near)


def body(features, seed_rows, hop1_ids, hop2_ids, w_self, w_neigh, bias, cotangent):
    sizes = [lax.axis_size(a) for a in GX_GY]
    split_x, split_z, split_y, split_c = sizes
    devices = split_x * split_z * split_y * split_c
    rows_dev, width = features.shape
    row_bits = rows_dev.bit_length() - 1
    hidden = w_self.shape[1]
    fan_one = hop1_ids.shape[1]
    fan_two = hop2_ids.shape[2]
    share = hidden // devices

    request, groups = plan(hop1_ids, hop2_ids, devices, row_bits)
    asked = exchange(request.reshape(devices, 1, SLOTS), GX_GY)
    served = serve(asked, features)
    rows = exchange(served.reshape(devices, MAIN, -1), GX_GY).reshape(devices * MAIN, -1)

    order = np.arange(hidden, dtype=np.int32).reshape(*sizes, share)
    order = np.transpose(order, (3, 0, 2, 1, 4)).reshape(1, hidden)
    turn = (lax.broadcasted_iota(jnp.int32, (hidden, hidden), 0) == jnp.asarray(order)).astype(BF16)
    self_turned = dot(w_self, turn).astype(BF16)
    neigh_turned = dot(w_neigh, turn).astype(BF16)
    bias_turned = bias[jnp.asarray(order[0])][None, :]
    spread = (cotangent.astype(F32) / (1 + fan_one)).astype(BF16)
    spread_turned = dot(spread, turn).astype(BF16)
    seed_x = features[seed_rows]
    main, far, near = slot_lanes(groups, devices)

    embedded_turned, grad = layer(
        rows, main, far, near, seed_x, self_turned, neigh_turned, bias_turned, spread_turned, fan_one, fan_two
    )
    embedded = dot(embedded_turned, turn, NT).astype(BF16)

    for axes, count in ((("gy_2",), split_c), (("gx", "gy_1"), split_x * split_y), (("gy_0",), split_z)):
        pieces = exchange(grad.reshape(count, -1, grad.shape[-1]), axes)
        grad = pieces.astype(F32).sum(axis=0)
        if axes != ("gy_0",):
            grad = grad.astype(BF16)
    return (embedded, grad[:, :width].T, grad[:, width : 2 * width].T, grad[:, 2 * width])


def solution(mesh):
    split = Mesh(mesh.devices.reshape(mesh.shape["gx"], 8, 4, 2), GX_GY)
    rows = P(GX_GY, None)
    in_specs = (rows, P(GX_GY), rows, P(GX_GY, None, None), P(), P(), P(), rows)
    out_specs = (rows, P(None, GX_GY), P(None, GX_GY), P(GX_GY))
    return jax.shard_map(body, mesh=split, in_specs=in_specs, out_specs=out_specs, check_vma=False)
```

```python
import functools

import jax
import jax.numpy as jnp
import numpy as np
from jax import lax
from jax.experimental import pallas as pl
from jax.experimental.pallas import tpu as pltpu
from jax.sharding import Mesh
from jax.sharding import PartitionSpec as P

GX_GY = ("gx", "gy_0", "gy_1", "gy_2")
FAR_CAP = 9
NEAR_CAP = 2
SLOTS = 16
MAIN = 8
EXTRA = 4
PLAN_BLOCK = 256
BF16 = jnp.bfloat16
F32 = jnp.float32
INTERPRET = False

NN = (((1,), (0,)), ((), ()))
NT = (((1,), (1,)), ((), ()))


def dot(left, right, dims=NN):
    return lax.dot_general(left, right, dims, preferred_element_type=F32)


def round_up(value, step):
    return -(-value // step) * step


def plan_kernel(devices, row_bits, far_blocks, ids_ref, base_ref, group_ref, request_ref, groups_ref):
    lanes = ids_ref.shape[1]
    block = PLAN_BLOCK
    upper = (
        lax.broadcasted_iota(jnp.int32, (block, block), 0) < lax.broadcasted_iota(jnp.int32, (block, block), 1)
    ).astype(F32).astype(BF16)
    owner_at = lax.broadcasted_iota(jnp.int32, (devices, block), 0)
    slot_at = lax.broadcasted_iota(jnp.int32, (SLOTS, block), 0)
    carry = jnp.zeros((devices, 1), F32)
    request = jnp.zeros((devices, SLOTS), F32)
    groups = jnp.zeros((devices, SLOTS), F32)
    for at in range(lanes // block):
        here = slice(at * block, (at + 1) * block)
        ids = ids_ref[:, here]
        if at == far_blocks:
            carry = jnp.zeros((devices, 1), F32)
        match = (owner_at == lax.shift_right_arithmetic(ids, row_bits)).astype(F32)
        match_low = match.astype(BF16)
        before = dot(match_low, upper) + carry
        carry = carry + jnp.sum(match, axis=1, keepdims=True)
        rank = jnp.sum(match * before, axis=0, keepdims=True)
        slot = rank.astype(jnp.int32) + base_ref[:, here]
        placed = (slot_at == slot).astype(F32)
        local = ids & ((1 << row_bits) - 1)
        low = local & 31
        group = group_ref[:, here]
        group_low = group & 31
        request = request + dot(match_low, (placed * (local - low).astype(F32)).astype(BF16), NT)
        request = request + dot(match_low, (placed * low.astype(F32)).astype(BF16), NT)
        groups = groups + dot(match_low, (placed * (group - group_low).astype(F32)).astype(BF16), NT)
        groups = groups + dot(match_low, (placed * group_low.astype(F32)).astype(BF16), NT)
    request_ref[...] = request.astype(jnp.int32)
    groups_ref[...] = groups.astype(jnp.int32) - 1


def plan(near_ids, far_ids, devices, row_bits):
    seeds, fan_one = near_ids.shape
    fan_two = far_ids.shape[2]
    far_total = seeds * fan_one * fan_two
    near_total = seeds * fan_one
    far_lanes = round_up(far_total, PLAN_BLOCK)
    near_lanes = round_up(near_total, PLAN_BLOCK)
    ids = jnp.concatenate(
        [
            jnp.pad(far_ids.reshape(1, -1), ((0, 0), (0, far_lanes - far_total)), constant_values=-1),
            jnp.pad(near_ids.reshape(1, -1), ((0, 0), (0, near_lanes - near_total)), constant_values=-1),
        ],
        axis=1,
    )
    lanes = far_lanes + near_lanes
    base = np.zeros((1, lanes), np.int32)
    base[:, far_lanes:] = FAR_CAP
    group = np.zeros((1, lanes), np.int32)
    far_at = np.arange(far_total)
    group[0, :far_total] = (far_at // fan_two) % fan_one * seeds + far_at // (fan_one * fan_two) + 1
    near_at = np.arange(near_total)
    group[0, far_lanes : far_lanes + near_total] = near_at % fan_one * seeds + near_at // fan_one + 1
    out = jax.ShapeDtypeStruct((devices, SLOTS), jnp.int32)
    return pl.pallas_call(
        lambda *refs: plan_kernel(devices, row_bits, far_lanes // PLAN_BLOCK, *refs),
        out_shape=(out, out),
        name="plan",
        interpret=INTERPRET,
    )(ids, jnp.asarray(base), jnp.asarray(group))


def halves_swapped(rows):
    return pltpu.roll(rows, EXTRA, axis=1)


def serve_kernel(asked_ref, features_ref, out_ref):
    peers = asked_ref.shape[0]
    rows_dev, width = features_ref.shape
    half = width // 2
    asked = asked_ref[...].astype(F32)

    def rows_of(asked, places, first):
        count = asked.shape[0]
        wide = jnp.broadcast_to(asked, (count, MAIN, SLOTS)) if asked.shape[1] == 1 else asked
        lane = lax.broadcasted_iota(jnp.int32, (count, MAIN, SLOTS), 2)
        place = lax.broadcasted_iota(jnp.int32, (count, MAIN, SLOTS), 1)
        chosen = jnp.sum(jnp.where(lane == first + place % places, wide, 0.0), axis=2, keepdims=True)
        row_at = lax.broadcasted_iota(jnp.int32, (count, MAIN, rows_dev), 2).astype(F32)
        picks = (row_at == chosen).astype(F32).reshape(count * MAIN, rows_dev).astype(BF16)
        return dot(picks, features_ref[...])

    out_ref[:, :width] = rows_of(asked, MAIN, 0).astype(BF16)
    pairs = asked.reshape(peers // 2, 2, 1, SLOTS)
    upper = lax.broadcasted_iota(jnp.int32, (peers // 2, MAIN, SLOTS), 1) < EXTRA
    both = jnp.where(
        upper,
        jnp.broadcast_to(pairs[:, 0], (peers // 2, MAIN, SLOTS)),
        jnp.broadcast_to(pairs[:, 1], (peers // 2, MAIN, SLOTS)),
    )
    extra = rows_of(both, EXTRA, MAIN).reshape(peers // 2, MAIN, width)
    left, right = extra[:, :, :half], extra[:, :, half:]
    upper = lax.broadcasted_iota(jnp.int32, (peers // 2, MAIN, half), 1) < EXTRA
    even = jnp.where(upper, left, halves_swapped(right))
    odd = jnp.where(upper, halves_swapped(left), right)
    packed = jnp.stack([even, odd], axis=1).reshape(peers * MAIN, half)
    out_ref[:, width:] = packed.astype(BF16)


def serve(asked, features, steps=8):
    devices = asked.shape[0]
    rows_dev, width = features.shape
    peers = devices // steps
    payload = width + width // 2
    return pl.pallas_call(
        serve_kernel,
        grid=(steps,),
        in_specs=[
            pl.BlockSpec((peers, 1, SLOTS), lambda i: (i, 0, 0)),
            pl.BlockSpec((rows_dev, width), lambda i: (0, 0)),
        ],
        out_specs=pl.BlockSpec((peers * MAIN, payload), lambda i: (i, 0)),
        out_shape=jax.ShapeDtypeStruct((devices * MAIN, payload), BF16),
        name="serve",
        interpret=INTERPRET,
    )(asked, features)


def unpack_kernel(steps, fan_one, fan_two, rows_ref, main_ref, far_ref, near_ref, seed_ref, out_ref, far_acc, near_acc):
    step = pl.program_id(0)
    seeds, width = seed_ref.shape
    half = width // 2
    near_total = near_acc.shape[0]
    lanes = rows_ref.shape[0]

    @pl.when(step == 0)
    def _():
        far_acc[...] = jnp.zeros_like(far_acc)
        near_acc[...] = jnp.zeros_like(near_acc)

    def picks(groups):
        group_at = lax.broadcasted_iota(jnp.int32, (near_total, groups.shape[1]), 0)
        return (group_at == groups).astype(F32).astype(BF16)

    packed = rows_ref[:, width:].astype(F32).reshape(lanes // (2 * MAIN), 2, MAIN, half)
    even, odd = packed[:, 0], packed[:, 1]
    upper = lax.broadcasted_iota(jnp.int32, even.shape, 1) < EXTRA
    left = jnp.where(upper, even, halves_swapped(odd)).reshape(lanes // 2, half)
    right = jnp.where(upper, halves_swapped(even), odd).reshape(lanes // 2, half)
    extra = jnp.concatenate([left, right], axis=1).astype(BF16)
    far_acc[...] += dot(picks(main_ref[...]), rows_ref[:, :width]) + dot(picks(far_ref[...]), extra)
    near_acc[...] += dot(picks(near_ref[...]), extra)

    @pl.when(step == steps - 1)
    def _():
        out_ref[:near_total, :width] = near_acc[...].astype(BF16)
        out_ref[near_total:, :width] = seed_ref[...]
        out_ref[:near_total, width:] = (far_acc[...] / fan_two).astype(BF16)
        summed = near_acc[:seeds]
        for k in range(1, fan_one):
            summed = summed + near_acc[k * seeds : (k + 1) * seeds]
        out_ref[near_total:, width:] = (summed / fan_one).astype(BF16)


def unpack(rows, main, far, near, seed_x, fan_one, fan_two, steps=4):
    total, payload = rows.shape
    seeds, width = seed_x.shape
    lanes = total // steps
    near_total = seeds * fan_one
    return pl.pallas_call(
        functools.partial(unpack_kernel, steps, fan_one, fan_two),
        grid=(steps,),
        in_specs=[
            pl.BlockSpec((lanes, payload), lambda i: (i, 0)),
            pl.BlockSpec((1, lanes), lambda i: (0, i)),
            pl.BlockSpec((1, lanes // 2), lambda i: (0, i)),
            pl.BlockSpec((1, lanes // 2), lambda i: (0, i)),
            pl.BlockSpec((seeds, width), lambda i: (0, 0)),
        ],
        out_specs=pl.BlockSpec((near_total + seeds, 2 * width), lambda i: (0, 0)),
        out_shape=jax.ShapeDtypeStruct((near_total + seeds, 2 * width), BF16),
        scratch_shapes=[pltpu.VMEM((near_total, width), F32), pltpu.VMEM((near_total, width), F32)],
        name="unpack",
        interpret=INTERPRET,
    )(rows, main, far, near, seed_x)


def layer_kernel(fan_one, own_ref, pair_ref, self_ref, neigh_ref, bias_ref, spread_ref, embedded_ref, grad_ref):
    seeds = spread_ref.shape[0] // 2
    width = self_ref.shape[0]
    near_total = seeds * fan_one
    turned = []
    for at, rows_ref in enumerate((own_ref, pair_ref)):
        pre = dot(rows_ref[:, :width], self_ref[...]) + dot(rows_ref[:, width:], neigh_ref[...]) + bias_ref[...]
        hidden = jnp.maximum(pre, 0.0).astype(BF16).astype(F32)
        summed = hidden[near_total:]
        for k in range(fan_one):
            summed = summed + hidden[k * seeds : (k + 1) * seeds]
        here = slice(at * seeds, (at + 1) * seeds)
        embedded_ref[here] = (summed / (1 + fan_one)).astype(BF16)
        spread = spread_ref[here].astype(F32)
        delta = jnp.where(pre > 0, jnp.concatenate([spread] * (1 + fan_one), axis=0), 0.0)
        turned.append(delta.T.astype(BF16))
    grad_ref[:, : 2 * width] = (dot(turned[0], own_ref[...]) + dot(turned[1], pair_ref[...])).astype(BF16)
    ones = (lax.broadcasted_iota(jnp.int32, (own_ref.shape[0], 128), 1) == 0).astype(F32).astype(BF16)
    grad_ref[:, 2 * width :] = (dot(turned[0], ones) + dot(turned[1], ones)).astype(BF16)


def layer(own, pair, w_self, w_neigh, bias, spread, fan_one, steps=2):
    rows, both = own.shape
    width, hidden = w_self.shape
    part = hidden // steps
    seeds = spread.shape[0]
    whole = pl.BlockSpec((rows, both), lambda i: (0, 0))
    weights = pl.BlockSpec((width, part), lambda i: (0, i))
    return pl.pallas_call(
        functools.partial(layer_kernel, fan_one),
        grid=(steps,),
        in_specs=[
            whole,
            whole,
            weights,
            weights,
            pl.BlockSpec((1, part), lambda i: (0, i)),
            pl.BlockSpec((seeds, part), lambda i: (0, i)),
        ],
        out_specs=(
            pl.BlockSpec((seeds, part), lambda i: (0, i)),
            pl.BlockSpec((part, both + 128), lambda i: (i, 0)),
        ),
        out_shape=(
            jax.ShapeDtypeStruct((seeds, hidden), BF16),
            jax.ShapeDtypeStruct((hidden, both + 128), BF16),
        ),
        name="layer",
        interpret=INTERPRET,
    )(own, pair, w_self, w_neigh, bias, spread)


def exchange(pieces, axes):
    return lax.all_to_all(pieces, axes, split_axis=0, concat_axis=0, tiled=True)


def swapped(x):
    return lax.ppermute(x, "gy_2", [(0, 1), (1, 0)])


def slot_lanes(groups):
    main = groups[:, :MAIN].reshape(1, -1)
    extra = groups[:, MAIN : MAIN + EXTRA]
    at = jnp.arange(EXTRA, dtype=jnp.int32)[None, :]
    far = jnp.where(at < FAR_CAP - MAIN, extra, -1)
    near = jnp.where(at >= FAR_CAP - MAIN, extra, -1)
    return main, far.reshape(1, -1), near.reshape(1, -1)


def body(features, seed_rows, hop1_ids, hop2_ids, w_self, w_neigh, bias, cotangent):
    sizes = [lax.axis_size(a) for a in GX_GY]
    split_x, split_z, split_y, split_c = sizes
    devices = split_x * split_z * split_y * split_c
    rows_dev, width = features.shape
    row_bits = rows_dev.bit_length() - 1
    hidden = w_self.shape[1]
    seeds, fan_one = hop1_ids.shape
    fan_two = hop2_ids.shape[2]
    share = hidden // devices

    request, groups = plan(hop1_ids, hop2_ids, devices, row_bits)
    asked = exchange(request.reshape(devices, 1, SLOTS), GX_GY)
    served = serve(asked, features)
    rows = exchange(served.reshape(devices, MAIN, -1), GX_GY).reshape(devices * MAIN, -1)

    order = np.arange(hidden, dtype=np.int32).reshape(*sizes, share)
    order = jnp.asarray(np.transpose(order, (3, 0, 2, 1, 4)).reshape(split_c, hidden // split_c))
    core = lax.axis_index("gy_2")
    unit = lax.broadcasted_iota(jnp.int32, (hidden, hidden // split_c), 0)
    hit = unit == lax.dynamic_index_in_dim(order, core, 0)
    turn = hit.astype(BF16)
    turn_other = (unit == lax.dynamic_index_in_dim(order, 1 - core, 0)).astype(BF16)
    self_turned = dot(w_self, turn).astype(BF16)
    neigh_turned = dot(w_neigh, turn).astype(BF16)
    bias_turned = jnp.sum(jnp.where(hit, bias[:, None], 0.0), axis=0)[None, :]
    spread = (cotangent.astype(F32) / (1 + fan_one)).astype(BF16)
    spread_turned = dot(jnp.concatenate([spread, swapped(spread)], axis=0), turn).astype(BF16)
    seed_x = features[seed_rows]

    made = (self_turned, neigh_turned, bias_turned, spread_turned, seed_x, *slot_lanes(groups))
    rows, made = lax.optimization_barrier((rows, made))
    turned, seed_x, lanes = made[:4], made[4], made[5:]
    own = unpack(rows, *lanes, seed_x, fan_one, fan_two)
    embedded, grad = layer(own, swapped(own), *turned, fan_one)
    embedded = (dot(embedded[:seeds], turn, NT) + dot(swapped(embedded[seeds:]), turn_other, NT)).astype(BF16)

    pieces = exchange(grad.reshape(split_x * split_y, -1, grad.shape[-1]), ("gx", "gy_1"))
    grad = pieces.astype(F32).sum(axis=0).astype(BF16)
    grad = exchange(grad.reshape(split_z, share, -1), ("gy_0",)).astype(F32).sum(axis=0)
    return (embedded, grad[:, :width].T, grad[:, width : 2 * width].T, grad[:, 2 * width])


def solution(mesh):
    split = Mesh(mesh.devices.reshape(mesh.shape["gx"], 8, 4, 2), GX_GY)
    rows = P(GX_GY, None)
    in_specs = (rows, P(GX_GY), rows, P(GX_GY, None, None), P(), P(), P(), rows)
    out_specs = (rows, P(None, GX_GY), P(None, GX_GY), P(GX_GY))
    return jax.shard_map(body, mesh=split, in_specs=in_specs, out_specs=out_specs, check_vma=False)
```

```python
import functools

import jax
import jax.numpy as jnp
import numpy as np
from jax import lax
from jax.experimental import pallas as pl
from jax.experimental.pallas import tpu as pltpu
from jax.sharding import Mesh
from jax.sharding import PartitionSpec as P

GX_GY = ("gx", "gy_0", "gy_1", "gy_2")
FAR_CAP = 9
NEAR_CAP = 2
SLOTS = 16
USED = FAR_CAP + NEAR_CAP
LANES = 128
PLAN_BLOCK = 256
BF16 = jnp.bfloat16
F32 = jnp.float32
INTERPRET = False

NN = (((1,), (0,)), ((), ()))
NT = (((1,), (1,)), ((), ()))


def dot(left, right, dims=NN):
    return lax.dot_general(left, right, dims, preferred_element_type=F32)


def round_up(value, step):
    return -(-value // step) * step


def plan_kernel(devices, row_bits, far_blocks, ids_ref, base_ref, group_ref, request_ref, groups_ref):
    lanes = ids_ref.shape[1]
    block = PLAN_BLOCK
    upper = (
        lax.broadcasted_iota(jnp.int32, (block, block), 0) < lax.broadcasted_iota(jnp.int32, (block, block), 1)
    ).astype(F32).astype(BF16)
    owner_at = lax.broadcasted_iota(jnp.int32, (devices, block), 0)
    slot_at = lax.broadcasted_iota(jnp.int32, (SLOTS, block), 0)
    carry = jnp.zeros((devices, 1), F32)
    found = jnp.zeros((4 * SLOTS, devices), F32)
    for at in range(lanes // block):
        here = slice(at * block, (at + 1) * block)
        ids = ids_ref[:, here]
        if at == far_blocks:
            carry = jnp.zeros((devices, 1), F32)
        match = (owner_at == lax.shift_right_arithmetic(ids, row_bits)).astype(F32)
        match_low = match.astype(BF16)
        before = dot(match_low, upper) + carry
        carry = carry + jnp.sum(match, axis=1, keepdims=True)
        rank = jnp.sum(match * before, axis=0, keepdims=True)
        slot = rank.astype(jnp.int32) + base_ref[:, here]
        placed = (slot_at == slot).astype(F32)
        local = ids & ((1 << row_bits) - 1)
        low = local & 31
        group = group_ref[:, here]
        group_low = group & 31
        values = (local - low, low, group - group_low, group_low)
        stacked = jnp.concatenate([placed * value.astype(F32) for value in values], axis=0).astype(BF16)
        found = found + dot(stacked, match_low, NT)
    request = found[:SLOTS] + found[SLOTS : 2 * SLOTS]
    groups = found[2 * SLOTS : 3 * SLOTS] + found[3 * SLOTS :]
    request_ref[...] = request.T.astype(jnp.int32)
    groups_ref[...] = groups.astype(jnp.int32) - 1


def plan(near_ids, far_ids, devices, row_bits):
    seeds, fan_one = near_ids.shape
    fan_two = far_ids.shape[2]
    far_total = seeds * fan_one * fan_two
    near_total = seeds * fan_one
    far_lanes = round_up(far_total, PLAN_BLOCK)
    near_lanes = round_up(near_total, PLAN_BLOCK)
    ids = jnp.concatenate(
        [
            jnp.pad(far_ids.reshape(1, -1), ((0, 0), (0, far_lanes - far_total)), constant_values=-1),
            jnp.pad(near_ids.reshape(1, -1), ((0, 0), (0, near_lanes - near_total)), constant_values=-1),
        ],
        axis=1,
    )
    lanes = far_lanes + near_lanes
    base = np.zeros((1, lanes), np.int32)
    base[:, far_lanes:] = FAR_CAP
    group = np.zeros((1, lanes), np.int32)
    far_at = np.arange(far_total)
    group[0, :far_total] = (far_at // fan_two) % fan_one * seeds + far_at // (fan_one * fan_two) + 1
    near_at = np.arange(near_total)
    group[0, far_lanes : far_lanes + near_total] = near_at % fan_one * seeds + near_at // fan_one + 1
    out = (jax.ShapeDtypeStruct((devices, SLOTS), jnp.int32), jax.ShapeDtypeStruct((SLOTS, devices), jnp.int32))
    return pl.pallas_call(
        lambda *refs: plan_kernel(devices, row_bits, far_lanes // PLAN_BLOCK, *refs),
        out_shape=out,
        name="plan",
        interpret=INTERPRET,
    )(ids, jnp.asarray(base), jnp.asarray(group))


def serve_kernel(asked_ref, features_ref, out_ref, spread_out):
    peers = asked_ref.shape[0]
    rows_dev, width = features_ref.shape
    pieces = width // LANES
    stride = USED * pieces
    asked = asked_ref[...].astype(F32)
    lane = lax.broadcasted_iota(jnp.int32, asked.shape, 1)
    row_at = lax.broadcasted_iota(jnp.int32, (peers, rows_dev), 1).astype(F32)
    picks = []
    for slot in range(USED):
        chosen = jnp.sum(jnp.where(lane == slot, asked, 0.0), axis=1, keepdims=True)
        picks.append((row_at == chosen).astype(F32).astype(BF16))
    found = dot(jnp.concatenate(picks, axis=0), features_ref[...])
    for slot in range(USED):
        rows = found[slot * peers : (slot + 1) * peers]
        for piece in range(pieces):
            spread_out[pl.ds(slot * pieces + piece, peers, stride=stride), :] = rows[:, piece * LANES : (piece + 1) * LANES]
    out_ref[...] = spread_out[...].astype(BF16)


def serve(asked, features, steps=4):
    devices = asked.shape[0]
    rows_dev, width = features.shape
    peers = devices // steps
    rows = USED * width // LANES
    return pl.pallas_call(
        serve_kernel,
        grid=(steps,),
        in_specs=[
            pl.BlockSpec((peers, SLOTS), lambda i: (i, 0)),
            pl.BlockSpec((rows_dev, width), lambda i: (0, 0)),
        ],
        out_specs=pl.BlockSpec((peers * rows, LANES), lambda i: (i, 0)),
        out_shape=jax.ShapeDtypeStruct((devices * rows, LANES), BF16),
        scratch_shapes=[pltpu.VMEM((peers * rows, LANES), F32)],
        name="serve",
        interpret=INTERPRET,
    )(asked, features)


def unpack_kernel(steps, fan_one, fan_two, rows_ref, groups_ref, seed_ref, out_ref, wide, far_acc, near_acc):
    step = pl.program_id(0)
    seeds, width = seed_ref.shape
    pieces = width // LANES
    stride = USED * pieces
    near_total = near_acc.shape[0]
    peers = groups_ref.shape[1]

    @pl.when(step == 0)
    def _():
        far_acc[...] = jnp.zeros_like(far_acc)
        near_acc[...] = jnp.zeros_like(near_acc)

    wide[...] = rows_ref[...].astype(F32)
    group_at = lax.broadcasted_iota(jnp.int32, (near_total, peers), 0)

    def taken(slots):
        rows, picks = [], []
        for slot in slots:
            at = [wide[pl.ds(slot * pieces + piece, peers, stride=stride), :] for piece in range(pieces)]
            rows.append(jnp.concatenate(at, axis=1).astype(BF16))
            picks.append((group_at == groups_ref[slot : slot + 1, :]).astype(F32).astype(BF16))
        return dot(jnp.concatenate(picks, axis=1), jnp.concatenate(rows, axis=0))

    far_acc[...] += taken(range(FAR_CAP))
    near_acc[...] += taken(range(FAR_CAP, USED))

    @pl.when(step == steps - 1)
    def _():
        out_ref[:near_total, :width] = near_acc[...].astype(BF16)
        out_ref[near_total:, :width] = seed_ref[...]
        out_ref[:near_total, width:] = (far_acc[...] / fan_two).astype(BF16)
        summed = near_acc[:seeds]
        for k in range(1, fan_one):
            summed = summed + near_acc[k * seeds : (k + 1) * seeds]
        out_ref[near_total:, width:] = (summed / fan_one).astype(BF16)


def unpack(rows, groups, seed_x, fan_one, fan_two, steps=2):
    total = rows.shape[0]
    seeds, width = seed_x.shape
    peers = groups.shape[1] // steps
    near_total = seeds * fan_one
    return pl.pallas_call(
        functools.partial(unpack_kernel, steps, fan_one, fan_two),
        grid=(steps,),
        in_specs=[
            pl.BlockSpec((total // steps, LANES), lambda i: (i, 0)),
            pl.BlockSpec((groups.shape[0], peers), lambda i: (0, i)),
            pl.BlockSpec((seeds, width), lambda i: (0, 0)),
        ],
        out_specs=pl.BlockSpec((near_total + seeds, 2 * width), lambda i: (0, 0)),
        out_shape=jax.ShapeDtypeStruct((near_total + seeds, 2 * width), BF16),
        scratch_shapes=[
            pltpu.VMEM((total // steps, LANES), F32),
            pltpu.VMEM((near_total, width), F32),
            pltpu.VMEM((near_total, width), F32),
        ],
        name="unpack",
        interpret=INTERPRET,
    )(rows, groups, seed_x)


def layer_kernel(fan_one, own_ref, pair_ref, self_ref, neigh_ref, bias_ref, spread_ref, embedded_ref, grad_ref):
    seeds = spread_ref.shape[0] // 2
    width = self_ref.shape[0]
    near_total = seeds * fan_one
    turned = []
    for at, rows_ref in enumerate((own_ref, pair_ref)):
        pre = dot(rows_ref[:, :width], self_ref[...]) + dot(rows_ref[:, width:], neigh_ref[...]) + bias_ref[...]
        hidden = jnp.maximum(pre, 0.0).astype(BF16).astype(F32)
        summed = hidden[near_total:]
        for k in range(fan_one):
            summed = summed + hidden[k * seeds : (k + 1) * seeds]
        here = slice(at * seeds, (at + 1) * seeds)
        embedded_ref[here] = (summed / (1 + fan_one)).astype(BF16)
        spread = spread_ref[here].astype(F32)
        delta = jnp.where(pre > 0, jnp.concatenate([spread] * (1 + fan_one), axis=0), 0.0)
        turned.append(delta.T.astype(BF16))
    grad_ref[:, : 2 * width] = (dot(turned[0], own_ref[...]) + dot(turned[1], pair_ref[...])).astype(BF16)
    ones = (lax.broadcasted_iota(jnp.int32, (own_ref.shape[0], 128), 1) == 0).astype(F32).astype(BF16)
    grad_ref[:, 2 * width :] = (dot(turned[0], ones) + dot(turned[1], ones)).astype(BF16)


def layer(own, pair, w_self, w_neigh, bias, spread, fan_one, steps=2):
    rows, both = own.shape
    width, hidden = w_self.shape
    part = hidden // steps
    seeds = spread.shape[0]
    whole = pl.BlockSpec((rows, both), lambda i: (0, 0))
    weights = pl.BlockSpec((width, part), lambda i: (0, i))
    return pl.pallas_call(
        functools.partial(layer_kernel, fan_one),
        grid=(steps,),
        in_specs=[
            whole,
            whole,
            weights,
            weights,
            pl.BlockSpec((1, part), lambda i: (0, i)),
            pl.BlockSpec((seeds, part), lambda i: (0, i)),
        ],
        out_specs=(
            pl.BlockSpec((seeds, part), lambda i: (0, i)),
            pl.BlockSpec((part, both + 128), lambda i: (i, 0)),
        ),
        out_shape=(
            jax.ShapeDtypeStruct((seeds, hidden), BF16),
            jax.ShapeDtypeStruct((hidden, both + 128), BF16),
        ),
        name="layer",
        interpret=INTERPRET,
    )(own, pair, w_self, w_neigh, bias, spread)


def exchange(pieces, axes):
    return lax.all_to_all(pieces, axes, split_axis=0, concat_axis=0, tiled=True)


def swapped(x):
    return lax.ppermute(x, "gy_2", [(0, 1), (1, 0)])


def body(features, seed_rows, hop1_ids, hop2_ids, w_self, w_neigh, bias, cotangent):
    sizes = [lax.axis_size(a) for a in GX_GY]
    split_x, split_z, split_y, split_c = sizes
    devices = split_x * split_z * split_y * split_c
    rows_dev, width = features.shape
    row_bits = rows_dev.bit_length() - 1
    hidden = w_self.shape[1]
    seeds, fan_one = hop1_ids.shape
    fan_two = hop2_ids.shape[2]
    share = hidden // devices

    request, groups = plan(hop1_ids, hop2_ids, devices, row_bits)
    asked = exchange(request.reshape(devices, 1, SLOTS), GX_GY).reshape(devices, SLOTS)
    served = serve(asked, features).reshape(devices, -1, 2, LANES)
    rows = exchange(served, GX_GY).reshape(-1, LANES)

    order = np.arange(hidden, dtype=np.int32).reshape(*sizes, share)
    order = jnp.asarray(np.transpose(order, (3, 0, 2, 1, 4)).reshape(split_c, hidden // split_c))
    core = lax.axis_index("gy_2")
    unit = lax.broadcasted_iota(jnp.int32, (hidden, hidden // split_c), 0)
    hit = unit == lax.dynamic_index_in_dim(order, core, 0)
    turn = hit.astype(BF16)
    turn_other = (unit == lax.dynamic_index_in_dim(order, 1 - core, 0)).astype(BF16)
    self_turned = dot(w_self, turn).astype(BF16)
    neigh_turned = dot(w_neigh, turn).astype(BF16)
    bias_turned = jnp.sum(jnp.where(hit, bias[:, None], 0.0), axis=0)[None, :]
    spread = (cotangent.astype(F32) / (1 + fan_one)).astype(BF16)
    spread_turned = dot(jnp.concatenate([spread, swapped(spread)], axis=0), turn).astype(BF16)
    seed_x = features[seed_rows]

    made = (self_turned, neigh_turned, bias_turned, spread_turned, seed_x, groups)
    rows, made = lax.optimization_barrier((rows, made))
    turned, seed_x, lanes = made[:4], made[4], made[5]
    own = unpack(rows, lanes, seed_x, fan_one, fan_two)
    embedded, grad = layer(own, swapped(own), *turned, fan_one)
    embedded = (dot(embedded[:seeds], turn, NT) + dot(swapped(embedded[seeds:]), turn_other, NT)).astype(BF16)

    pieces = exchange(grad.reshape(split_x * split_y, -1, grad.shape[-1]), ("gx", "gy_1"))
    grad = pieces.astype(F32).sum(axis=0).astype(BF16)
    grad = exchange(grad.reshape(split_z, share, -1), ("gy_0",)).astype(F32).sum(axis=0)
    return (embedded, grad[:, :width].T, grad[:, width : 2 * width].T, grad[:, 2 * width])


def solution(mesh):
    split = Mesh(mesh.devices.reshape(mesh.shape["gx"], 8, 4, 2), GX_GY)
    rows = P(GX_GY, None)
    in_specs = (rows, P(GX_GY), rows, P(GX_GY, None, None), P(), P(), P(), rows)
    out_specs = (rows, P(None, GX_GY), P(None, GX_GY), P(GX_GY))
    return jax.shard_map(body, mesh=split, in_specs=in_specs, out_specs=out_specs, check_vma=False)
```

```python
import functools

import jax
import jax.numpy as jnp
import numpy as np
from jax import lax
from jax.experimental import pallas as pl
from jax.experimental.pallas import tpu as pltpu
from jax.sharding import Mesh
from jax.sharding import PartitionSpec as P

GX_GY = ("gx", "gy_0", "gy_1", "gy_2")
FAR_CAP = 9
NEAR_CAP = 2
SLOTS = 16
USED = FAR_CAP + NEAR_CAP
LANES = 128
PLAN_BLOCK = 256
BF16 = jnp.bfloat16
F32 = jnp.float32
INTERPRET = False

NN = (((1,), (0,)), ((), ()))
NT = (((1,), (1,)), ((), ()))


def dot(left, right, dims=NN):
    return lax.dot_general(left, right, dims, preferred_element_type=F32)


def round_up(value, step):
    return -(-value // step) * step


def plan_kernel(devices, row_bits, far_ref, near_ref, request_ref, groups_ref):
    fan_one, fan_two, seeds = far_ref.shape
    block = PLAN_BLOCK
    upper = (
        lax.broadcasted_iota(jnp.int32, (block, block), 0) < lax.broadcasted_iota(jnp.int32, (block, block), 1)
    ).astype(F32).astype(BF16)
    owner_at = lax.broadcasted_iota(jnp.int32, (devices, block), 0)
    slot_at = lax.broadcasted_iota(jnp.int32, (SLOTS, block), 0)
    lane = lax.broadcasted_iota(jnp.int32, (1, block), 1)
    found = jnp.zeros((4 * SLOTS, devices), F32)
    far = [(k, far_ref[k, j : j + 1, :]) for k in range(fan_one) for j in range(fan_two)]
    near = [(k, near_ref[k : k + 1, :]) for k in range(fan_one)]
    for first, pieces in ((0, far), (FAR_CAP, near)):
        carry = jnp.zeros((devices, 1), F32)
        for at in range(0, len(pieces), block // seeds):
            here = pieces[at : at + block // seeds]
            rest = block // seeds - len(here)
            ids = jnp.concatenate([ids for _, ids in here] + [jnp.full((1, seeds), -1, jnp.int32)] * rest, axis=1)
            group = lane % seeds + 1
            for place, (k, _) in enumerate(here):
                group = group + jnp.where(lane // seeds == place, k * seeds, 0)
            match = (owner_at == lax.shift_right_arithmetic(ids, row_bits)).astype(F32)
            match_low = match.astype(BF16)
            before = dot(match_low, upper) + carry
            carry = carry + jnp.sum(match, axis=1, keepdims=True)
            rank = jnp.sum(match * before, axis=0, keepdims=True)
            placed = (slot_at == rank.astype(jnp.int32) + first).astype(F32)
            local = ids & ((1 << row_bits) - 1)
            low = local & 31
            group_low = group & 31
            values = (local - low, low, group - group_low, group_low)
            stacked = jnp.concatenate([placed * value.astype(F32) for value in values], axis=0).astype(BF16)
            found = found + dot(stacked, match_low, NT)
    request = found[:SLOTS] + found[SLOTS : 2 * SLOTS]
    groups = found[2 * SLOTS : 3 * SLOTS] + found[3 * SLOTS :]
    request_ref[...] = request.T.astype(jnp.int32)
    groups_ref[...] = groups.astype(jnp.int32) - 1


def plan(near_ids, far_ids, devices, row_bits):
    out = (jax.ShapeDtypeStruct((devices, SLOTS), jnp.int32), jax.ShapeDtypeStruct((SLOTS, devices), jnp.int32))
    return pl.pallas_call(
        functools.partial(plan_kernel, devices, row_bits),
        out_shape=out,
        name="plan",
        interpret=INTERPRET,
    )(jnp.transpose(far_ids, (1, 2, 0)), jnp.transpose(near_ids))


def serve_kernel(asked_ref, features_ref, out_ref, spread_out):
    peers = asked_ref.shape[0]
    rows_dev, width = features_ref.shape
    pieces = width // LANES
    stride = USED * pieces
    asked = asked_ref[...].astype(F32)
    lane = lax.broadcasted_iota(jnp.int32, asked.shape, 1)
    row_at = lax.broadcasted_iota(jnp.int32, (peers, rows_dev), 1).astype(F32)
    picks = []
    for slot in range(USED):
        chosen = jnp.sum(jnp.where(lane == slot, asked, 0.0), axis=1, keepdims=True)
        picks.append((row_at == chosen).astype(F32).astype(BF16))
    found = dot(jnp.concatenate(picks, axis=0), features_ref[...])
    for slot in range(USED):
        rows = found[slot * peers : (slot + 1) * peers]
        for piece in range(pieces):
            spread_out[pl.ds(slot * pieces + piece, peers, stride=stride), :] = rows[:, piece * LANES : (piece + 1) * LANES]
    out_ref[...] = spread_out[...].astype(BF16)


def serve(asked, features, steps=4):
    devices = asked.shape[0]
    rows_dev, width = features.shape
    peers = devices // steps
    rows = USED * width // LANES
    return pl.pallas_call(
        serve_kernel,
        grid=(steps,),
        in_specs=[
            pl.BlockSpec((peers, SLOTS), lambda i: (i, 0)),
            pl.BlockSpec((rows_dev, width), lambda i: (0, 0)),
        ],
        out_specs=pl.BlockSpec((peers * rows, LANES), lambda i: (i, 0)),
        out_shape=jax.ShapeDtypeStruct((devices * rows, LANES), BF16),
        scratch_shapes=[pltpu.VMEM((peers * rows, LANES), F32)],
        name="serve",
        interpret=INTERPRET,
    )(asked, features)


def unpack_kernel(steps, fan_one, fan_two, rows_ref, groups_ref, seed_ref, out_ref, wide, far_acc, near_acc):
    step = pl.program_id(0)
    seeds, width = seed_ref.shape
    pieces = width // LANES
    stride = USED * pieces
    near_total = near_acc.shape[0]
    peers = groups_ref.shape[1]

    @pl.when(step == 0)
    def _():
        far_acc[...] = jnp.zeros_like(far_acc)
        near_acc[...] = jnp.zeros_like(near_acc)

    wide[...] = rows_ref[...].astype(F32)
    group_at = lax.broadcasted_iota(jnp.int32, (near_total, peers), 0)

    def taken(slots):
        rows, picks = [], []
        for slot in slots:
            at = [wide[pl.ds(slot * pieces + piece, peers, stride=stride), :] for piece in range(pieces)]
            rows.append(jnp.concatenate(at, axis=1).astype(BF16))
            picks.append((group_at == groups_ref[slot : slot + 1, :]).astype(F32).astype(BF16))
        return dot(jnp.concatenate(picks, axis=1), jnp.concatenate(rows, axis=0))

    far_acc[...] += taken(range(FAR_CAP))
    near_acc[...] += taken(range(FAR_CAP, USED))

    @pl.when(step == steps - 1)
    def _():
        out_ref[:near_total, :width] = near_acc[...].astype(BF16)
        out_ref[near_total:, :width] = seed_ref[...]
        out_ref[:near_total, width:] = (far_acc[...] / fan_two).astype(BF16)
        summed = near_acc[:seeds]
        for k in range(1, fan_one):
            summed = summed + near_acc[k * seeds : (k + 1) * seeds]
        out_ref[near_total:, width:] = (summed / fan_one).astype(BF16)


def unpack(rows, groups, seed_x, fan_one, fan_two, steps=2):
    total = rows.shape[0]
    seeds, width = seed_x.shape
    peers = groups.shape[1] // steps
    near_total = seeds * fan_one
    return pl.pallas_call(
        functools.partial(unpack_kernel, steps, fan_one, fan_two),
        grid=(steps,),
        in_specs=[
            pl.BlockSpec((total // steps, LANES), lambda i: (i, 0)),
            pl.BlockSpec((groups.shape[0], peers), lambda i: (0, i)),
            pl.BlockSpec((seeds, width), lambda i: (0, 0)),
        ],
        out_specs=pl.BlockSpec((near_total + seeds, 2 * width), lambda i: (0, 0)),
        out_shape=jax.ShapeDtypeStruct((near_total + seeds, 2 * width), BF16),
        scratch_shapes=[
            pltpu.VMEM((total // steps, LANES), F32),
            pltpu.VMEM((near_total, width), F32),
            pltpu.VMEM((near_total, width), F32),
        ],
        name="unpack",
        interpret=INTERPRET,
    )(rows, groups, seed_x)


def layer_kernel(fan_one, rows_ref, self_ref, neigh_ref, bias_ref, spread_ref, *refs):
    *earlier, embedded_ref, grad_ref = refs
    seeds = spread_ref.shape[0]
    width = self_ref.shape[0]
    near_total = seeds * fan_one
    pre = dot(rows_ref[:, :width], self_ref[...]) + dot(rows_ref[:, width:], neigh_ref[...]) + bias_ref[...]
    hidden = jnp.maximum(pre, 0.0).astype(BF16).astype(F32)
    summed = hidden[near_total:]
    for k in range(fan_one):
        summed = summed + hidden[k * seeds : (k + 1) * seeds]
    embedded_ref[...] = (summed / (1 + fan_one)).astype(BF16)
    spread = spread_ref[...].astype(F32)
    delta = jnp.where(pre > 0, jnp.concatenate([spread] * (1 + fan_one), axis=0), 0.0)
    turned = delta.T.astype(BF16)
    ones = (lax.broadcasted_iota(jnp.int32, (rows_ref.shape[0], LANES), 1) == 0).astype(F32).astype(BF16)
    for start, part in ((0, rows_ref[...]), (2 * width, ones)):
        here = slice(start, start + part.shape[1])
        grad = dot(turned, part)
        for ref in earlier:
            grad = grad + ref[:, here]
        grad_ref[:, here] = grad.astype(grad_ref.dtype)


def layer(rows, w_self, w_neigh, bias, spread, fan_one, earlier=(), steps=2):
    count, both = rows.shape
    width, hidden = w_self.shape
    part = hidden // steps
    seeds = spread.shape[0]
    weights = pl.BlockSpec((width, part), lambda i: (0, i))
    grads = pl.BlockSpec((part, both + LANES), lambda i: (i, 0))
    return pl.pallas_call(
        functools.partial(layer_kernel, fan_one),
        grid=(steps,),
        in_specs=[
            pl.BlockSpec((count, both), lambda i: (0, 0)),
            weights,
            weights,
            pl.BlockSpec((1, part), lambda i: (0, i)),
            pl.BlockSpec((seeds, part), lambda i: (0, i)),
            *[grads for _ in earlier],
        ],
        out_specs=(pl.BlockSpec((seeds, part), lambda i: (0, i)), grads),
        out_shape=(
            jax.ShapeDtypeStruct((seeds, hidden), BF16),
            jax.ShapeDtypeStruct((hidden, both + LANES), BF16 if earlier else F32),
        ),
        name="layer_second" if earlier else "layer_first",
        interpret=INTERPRET,
    )(rows, w_self, w_neigh, bias, spread, *earlier)


def last_kernel(pieces_ref, self_ref, neigh_ref, bias_ref):
    share, width = self_ref.shape
    summed = pieces_ref[0].astype(F32)
    for at in range(1, pieces_ref.shape[0]):
        summed = summed + pieces_ref[at].astype(F32)
    self_ref[...] = summed[:, :width]
    neigh_ref[...] = summed[:, width : 2 * width]
    square = (share, share)
    here = lax.broadcasted_iota(jnp.int32, square, 0) == lax.broadcasted_iota(jnp.int32, square, 1)
    column = jnp.broadcast_to(summed[:, 2 * width : 2 * width + 1], square)
    bias_ref[...] = jnp.sum(jnp.where(here, column, 0.0), axis=0, keepdims=True)


def last(pieces, width):
    share = pieces.shape[1]
    return pl.pallas_call(
        last_kernel,
        out_shape=(
            jax.ShapeDtypeStruct((share, width), F32),
            jax.ShapeDtypeStruct((share, width), F32),
            jax.ShapeDtypeStruct((1, share), F32),
        ),
        name="last",
        interpret=INTERPRET,
    )(pieces)


def exchange(pieces, axes):
    return lax.all_to_all(pieces, axes, split_axis=0, concat_axis=0, tiled=True)


def swapped(x):
    return lax.ppermute(x, "gy_2", [(0, 1), (1, 0)])


def body(features, seed_rows, hop1_ids, hop2_ids, w_self, w_neigh, bias, cotangent):
    sizes = [lax.axis_size(a) for a in GX_GY]
    split_x, split_z, split_y, split_c = sizes
    devices = split_x * split_z * split_y * split_c
    rows_dev, width = features.shape
    row_bits = rows_dev.bit_length() - 1
    hidden = w_self.shape[1]
    seeds, fan_one = hop1_ids.shape
    fan_two = hop2_ids.shape[2]
    share = hidden // devices

    request, groups = plan(hop1_ids, hop2_ids, devices, row_bits)
    asked = exchange(request.reshape(devices, 1, SLOTS), GX_GY).reshape(devices, SLOTS)
    served = serve(asked, features).reshape(devices, -1, 2, LANES)
    rows = exchange(served, GX_GY).reshape(-1, LANES)

    order = np.arange(hidden, dtype=np.int32).reshape(*sizes, share)
    order = jnp.asarray(np.transpose(order, (3, 0, 2, 1, 4)).reshape(split_c, hidden // split_c))
    core = lax.axis_index("gy_2")
    unit = lax.broadcasted_iota(jnp.int32, (hidden, hidden // split_c), 0)
    hit = unit == lax.dynamic_index_in_dim(order, core, 0)
    turn = hit.astype(BF16)
    turn_other = (unit == lax.dynamic_index_in_dim(order, 1 - core, 0)).astype(BF16)
    self_turned = dot(w_self, turn).astype(BF16)
    neigh_turned = dot(w_neigh, turn).astype(BF16)
    bias_turned = jnp.sum(jnp.where(hit, bias[:, None], 0.0), axis=0)[None, :]
    spread = (cotangent.astype(F32) / (1 + fan_one)).astype(BF16)
    spread_turned = dot(jnp.concatenate([spread, swapped(spread)], axis=0), turn).astype(BF16)
    seed_x = features[seed_rows]

    made = (self_turned, neigh_turned, bias_turned, spread_turned, seed_x, groups)
    rows, made = lax.optimization_barrier((rows, made))
    turned, seed_x, lanes = made[:4], made[4], made[5]
    own = unpack(rows, lanes, seed_x, fan_one, fan_two)
    *turned, spread_turned = turned
    pair = swapped(own)
    embedded_own, grad = layer(own, *turned, spread_turned[:seeds], fan_one)
    embedded_pair, grad = layer(pair, *turned, spread_turned[seeds:], fan_one, (grad,))
    embedded = (dot(embedded_own, turn, NT) + dot(swapped(embedded_pair), turn_other, NT)).astype(BF16)

    pieces = exchange(grad.reshape(split_x * split_y, -1, grad.shape[-1]), ("gx", "gy_1"))
    grad = pieces.astype(F32).sum(axis=0).astype(BF16)
    pieces = exchange(grad.reshape(split_z, share, -1), ("gy_0",))
    grad_self, grad_neigh, grad_bias = last(pieces, width)
    return (embedded, grad_self.T, grad_neigh.T, grad_bias.reshape(-1))


def solution(mesh):
    split = Mesh(mesh.devices.reshape(mesh.shape["gx"], 8, 4, 2), GX_GY)
    rows = P(GX_GY, None)
    in_specs = (rows, P(GX_GY), rows, P(GX_GY, None, None), P(), P(), P(), rows)
    out_specs = (rows, P(None, GX_GY), P(None, GX_GY), P(GX_GY))
    return jax.shard_map(body, mesh=split, in_specs=in_specs, out_specs=out_specs, check_vma=False)
```

```python
import functools

import jax
import jax.numpy as jnp
import numpy as np
from jax import lax
from jax.experimental import pallas as pl
from jax.experimental.pallas import tpu as pltpu
from jax.sharding import Mesh
from jax.sharding import PartitionSpec as P

GX_GY = ("gx", "gy_0", "gy_1", "gy_2")
FAR_CAP = 9
NEAR_CAP = 2
SLOTS = 16
USED = FAR_CAP + NEAR_CAP
LANES = 128
PLAN_BLOCK = 256
BF16 = jnp.bfloat16
F32 = jnp.float32
INTERPRET = False
KERNEL_VMEM = 40 << 20

NN = (((1,), (0,)), ((), ()))
NT = (((1,), (1,)), ((), ()))


def dot(left, right, dims=NN):
    return lax.dot_general(left, right, dims, preferred_element_type=F32)


ON_CHIP = pl.BlockSpec(memory_space=pltpu.VMEM)


def on_chip(x):
    return pltpu.with_memory_space_constraint(x, pltpu.VMEM)


def plan_kernel(
    devices, row_bits, far_hbm, near_hbm, features_hbm, request_ref, groups_ref, held_ref, far_ref, near_ref, arrived
):
    pairs = ((far_hbm, far_ref), (near_hbm, near_ref), (features_hbm, held_ref))
    copies = [pltpu.make_async_copy(*pair, arrived.at[at]) for at, pair in enumerate(pairs)]
    for copy in copies:
        copy.start()
    for copy in copies[:2]:
        copy.wait()
    fan_one, fan_two, seeds = far_ref.shape
    block = PLAN_BLOCK
    upper = (
        lax.broadcasted_iota(jnp.int32, (block, block), 0) < lax.broadcasted_iota(jnp.int32, (block, block), 1)
    ).astype(F32).astype(BF16)
    owner_at = lax.broadcasted_iota(jnp.int32, (devices, block), 0)
    slot_at = lax.broadcasted_iota(jnp.int32, (SLOTS, block), 0)
    lane = lax.broadcasted_iota(jnp.int32, (1, block), 1)
    found = jnp.zeros((4 * SLOTS, devices), F32)
    far = [(k, far_ref[k, j : j + 1, :]) for k in range(fan_one) for j in range(fan_two)]
    near = [(k, near_ref[k : k + 1, :]) for k in range(fan_one)]
    for first, pieces in ((0, far), (FAR_CAP, near)):
        carry = jnp.zeros((devices, 1), F32)
        for at in range(0, len(pieces), block // seeds):
            here = pieces[at : at + block // seeds]
            rest = block // seeds - len(here)
            ids = jnp.concatenate([ids for _, ids in here] + [jnp.full((1, seeds), -1, jnp.int32)] * rest, axis=1)
            group = lane % seeds + 1
            for place, (k, _) in enumerate(here):
                group = group + jnp.where(lane // seeds == place, k * seeds, 0)
            match = (owner_at == lax.shift_right_arithmetic(ids, row_bits)).astype(F32)
            match_low = match.astype(BF16)
            before = dot(match_low, upper) + carry
            carry = carry + jnp.sum(match, axis=1, keepdims=True)
            rank = jnp.sum(match * before, axis=0, keepdims=True)
            placed = (slot_at == rank.astype(jnp.int32) + first).astype(F32)
            local = ids & ((1 << row_bits) - 1)
            low = local & 31
            group_low = group & 31
            values = (local - low, low, group - group_low, group_low)
            stacked = jnp.concatenate([placed * value.astype(F32) for value in values], axis=0).astype(BF16)
            found = found + dot(stacked, match_low, NT)
    request = found[:SLOTS] + found[SLOTS : 2 * SLOTS]
    groups = found[2 * SLOTS : 3 * SLOTS] + found[3 * SLOTS :]
    request_ref[...] = request.T.astype(jnp.int32)
    groups_ref[...] = groups.astype(jnp.int32) - 1
    copies[2].wait()


def plan(near_ids, far_ids, features, devices, row_bits):
    out = (
        jax.ShapeDtypeStruct((devices, SLOTS), jnp.int32),
        jax.ShapeDtypeStruct((SLOTS, devices), jnp.int32),
        pltpu.VMEM(features.shape, features.dtype),
    )
    far_ids, near_ids = jnp.transpose(far_ids, (1, 2, 0)), jnp.transpose(near_ids)
    inputs = [pltpu.with_memory_space_constraint(x, pltpu.HBM) for x in (far_ids, near_ids, features)]
    return pl.pallas_call(
        functools.partial(plan_kernel, devices, row_bits),
        in_specs=[pl.BlockSpec(memory_space=pltpu.HBM)] * 3,
        out_specs=(ON_CHIP,) * 3,
        out_shape=out,
        scratch_shapes=[
            pltpu.VMEM(far_ids.shape, jnp.int32),
            pltpu.VMEM(near_ids.shape, jnp.int32),
            pltpu.SemaphoreType.DMA((3,)),
        ],
        compiler_params=pltpu.CompilerParams(vmem_limit_bytes=KERNEL_VMEM),
        name="plan",
        interpret=INTERPRET,
    )(*inputs)


def serve_kernel(asked_ref, features_ref, out_ref, spread_out):
    peers = asked_ref.shape[0]
    rows_dev, width = features_ref.shape
    pieces = width // LANES
    stride = USED * pieces
    asked = asked_ref[...].astype(F32)
    lane = lax.broadcasted_iota(jnp.int32, asked.shape, 1)
    row_at = lax.broadcasted_iota(jnp.int32, (peers, rows_dev), 1).astype(F32)
    picks = []
    for slot in range(USED):
        chosen = jnp.sum(jnp.where(lane == slot, asked, 0.0), axis=1, keepdims=True)
        picks.append((row_at == chosen).astype(F32).astype(BF16))
    found = dot(jnp.concatenate(picks, axis=0), features_ref[...])
    for slot in range(USED):
        rows = found[slot * peers : (slot + 1) * peers]
        for piece in range(pieces):
            spread_out[pl.ds(slot * pieces + piece, peers, stride=stride), :] = rows[:, piece * LANES : (piece + 1) * LANES]
    out_ref[...] = spread_out[...].astype(BF16)


def serve(asked, features, steps=4):
    devices = asked.shape[0]
    rows_dev, width = features.shape
    peers = devices // steps
    rows = USED * width // LANES
    return pl.pallas_call(
        serve_kernel,
        grid=(steps,),
        in_specs=[
            pl.BlockSpec((peers, SLOTS), lambda i: (i, 0)),
            ON_CHIP,
        ],
        out_specs=pl.BlockSpec((peers * rows, LANES), lambda i: (i, 0)),
        out_shape=pltpu.HBM((devices * rows, LANES), BF16),
        scratch_shapes=[pltpu.VMEM((peers * rows, LANES), F32)],
        compiler_params=pltpu.CompilerParams(vmem_limit_bytes=KERNEL_VMEM),
        name="serve",
        interpret=INTERPRET,
    )(asked, on_chip(features))


def unpack_kernel(steps, fan_one, fan_two, rows_ref, groups_ref, seed_ref, out_ref, wide, far_acc, near_acc):
    step = pl.program_id(0)
    seeds, width = seed_ref.shape
    pieces = width // LANES
    stride = USED * pieces
    near_total = near_acc.shape[0]
    peers = groups_ref.shape[1]

    @pl.when(step == 0)
    def _():
        far_acc[...] = jnp.zeros_like(far_acc)
        near_acc[...] = jnp.zeros_like(near_acc)

    wide[...] = rows_ref[...].astype(F32)
    group_at = lax.broadcasted_iota(jnp.int32, (near_total, peers), 0)

    def taken(slots):
        rows, picks = [], []
        for slot in slots:
            at = [wide[pl.ds(slot * pieces + piece, peers, stride=stride), :] for piece in range(pieces)]
            rows.append(jnp.concatenate(at, axis=1).astype(BF16))
            picks.append((group_at == groups_ref[slot : slot + 1, :]).astype(F32).astype(BF16))
        return dot(jnp.concatenate(picks, axis=1), jnp.concatenate(rows, axis=0))

    far_acc[...] += taken(range(FAR_CAP))
    near_acc[...] += taken(range(FAR_CAP, USED))

    @pl.when(step == steps - 1)
    def _():
        out_ref[:near_total, :width] = near_acc[...].astype(BF16)
        out_ref[near_total:, :width] = seed_ref[...]
        out_ref[:near_total, width:] = (far_acc[...] / fan_two).astype(BF16)
        summed = near_acc[:seeds]
        for k in range(1, fan_one):
            summed = summed + near_acc[k * seeds : (k + 1) * seeds]
        out_ref[near_total:, width:] = (summed / fan_one).astype(BF16)


def unpack(rows, groups, seed_x, fan_one, fan_two, steps=2):
    total = rows.shape[0]
    seeds, width = seed_x.shape
    peers = groups.shape[1] // steps
    near_total = seeds * fan_one
    return pl.pallas_call(
        functools.partial(unpack_kernel, steps, fan_one, fan_two),
        grid=(steps,),
        in_specs=[
            pl.BlockSpec((total // steps, LANES), lambda i: (i, 0)),
            pl.BlockSpec((groups.shape[0], peers), lambda i: (0, i)),
            pl.BlockSpec((seeds, width), lambda i: (0, 0)),
        ],
        out_specs=ON_CHIP,
        out_shape=pltpu.VMEM((near_total + seeds, 2 * width), BF16),
        scratch_shapes=[
            pltpu.VMEM((total // steps, LANES), F32),
            pltpu.VMEM((near_total, width), F32),
            pltpu.VMEM((near_total, width), F32),
        ],
        compiler_params=pltpu.CompilerParams(vmem_limit_bytes=KERNEL_VMEM),
        name="unpack",
        interpret=INTERPRET,
    )(rows, groups, seed_x)


def forward(fan_one, rows_ref, self_ref, neigh_ref, bias_ref, spread_ref, embedded_ref):
    seeds = spread_ref.shape[0]
    width = self_ref.shape[0]
    near_total = seeds * fan_one
    pre = dot(rows_ref[:, :width], self_ref[...]) + dot(rows_ref[:, width:], neigh_ref[...]) + bias_ref[...]
    hidden = jnp.maximum(pre, 0.0).astype(BF16).astype(F32)
    summed = hidden[near_total:]
    for k in range(fan_one):
        summed = summed + hidden[k * seeds : (k + 1) * seeds]
    embedded_ref[...] = (summed / (1 + fan_one)).astype(BF16)
    spread = spread_ref[...].astype(F32)
    return jnp.where(pre > 0, jnp.concatenate([spread] * (1 + fan_one), axis=0), 0.0).T


def first_kernel(fan_one, part, rows_ref, self_ref, neigh_ref, bias_ref, spread_ref, embedded_ref, turned_ref):
    here = pl.ds(pl.multiple_of(pl.program_id(0) * part, part), part)
    turned = forward(fan_one, rows_ref, self_ref, neigh_ref, bias_ref, spread_ref, embedded_ref)
    turned_ref[here, :] = turned.astype(BF16)


def second_kernel(
    fan_one, part, rows_ref, self_ref, neigh_ref, bias_ref, spread_ref, own_ref, turned_ref, embedded_ref, grad_ref, both
):
    count, columns = own_ref.shape
    here = pl.ds(pl.multiple_of(pl.program_id(0) * part, part), part)

    @pl.when(pl.program_id(0) == 0)
    def _():
        both[:count] = own_ref[...]
        both[count:] = rows_ref[...]

    pair = forward(fan_one, rows_ref, self_ref, neigh_ref, bias_ref, spread_ref, embedded_ref)
    turned = jnp.concatenate([turned_ref[here, :], pair.astype(BF16)], axis=1)
    grad_ref[:, :columns] = dot(turned, both[...]).astype(BF16)
    summed = jnp.sum(turned.astype(F32), axis=1, keepdims=True)
    grad_ref[:, columns:] = jnp.broadcast_to(summed, (part, LANES)).astype(BF16)


def layer(rows, w_self, w_neigh, bias, spread, fan_one, own=(), steps=2):
    count, both = rows.shape
    width, hidden = w_self.shape
    part = hidden // steps
    seeds = spread.shape[0]
    weights = pl.BlockSpec((width, part), lambda i: (0, i))
    half = pl.BlockSpec((seeds, part), lambda i: (0, i))
    if own:
        last_spec = pl.BlockSpec((part, both + LANES), lambda i: (i, 0))
        last_shape = pltpu.HBM((hidden, both + LANES), BF16)
    else:
        last_spec = ON_CHIP
        last_shape = pltpu.VMEM((hidden, count), BF16)
    return pl.pallas_call(
        functools.partial(second_kernel if own else first_kernel, fan_one, part),
        grid=(steps,),
        in_specs=[
            ON_CHIP,
            weights,
            weights,
            pl.BlockSpec((1, part), lambda i: (0, i)),
            half,
            *[ON_CHIP for _ in own],
        ],
        out_specs=(half, last_spec),
        out_shape=(jax.ShapeDtypeStruct((seeds, hidden), BF16), last_shape),
        scratch_shapes=[pltpu.VMEM((2 * count, both), BF16)] if own else [],
        compiler_params=pltpu.CompilerParams(vmem_limit_bytes=KERNEL_VMEM),
        name="layer_second" if own else "layer_first",
        interpret=INTERPRET,
    )(on_chip(rows), w_self, w_neigh, bias, spread, *[on_chip(x) for x in own])


def sum_kernel(pieces_ref, out_ref):
    summed = pieces_ref[0].astype(F32)
    for at in range(1, pieces_ref.shape[0]):
        summed = summed + pieces_ref[at].astype(F32)
    out_ref[...] = summed.reshape(out_ref.shape).astype(BF16)


def sum_pieces(pieces, groups):
    _, rows, columns = pieces.shape
    return pl.pallas_call(
        sum_kernel,
        in_specs=[ON_CHIP],
        out_specs=ON_CHIP,
        out_shape=pltpu.VMEM((groups, rows // groups, columns), BF16),
        compiler_params=pltpu.CompilerParams(vmem_limit_bytes=KERNEL_VMEM),
        name="sum_pieces",
        interpret=INTERPRET,
    )(on_chip(pieces))


def exchange(pieces, axes):
    return lax.all_to_all(pieces, axes, split_axis=0, concat_axis=0, tiled=True)


def swapped(x):
    return lax.ppermute(x, "gy_2", [(0, 1), (1, 0)])


def body(features, seed_rows, hop1_ids, hop2_ids, w_self, w_neigh, bias, cotangent):
    sizes = [lax.axis_size(a) for a in GX_GY]
    split_x, split_z, split_y, split_c = sizes
    devices = split_x * split_z * split_y * split_c
    rows_dev, width = features.shape
    row_bits = rows_dev.bit_length() - 1
    hidden = w_self.shape[1]
    seeds, fan_one = hop1_ids.shape
    fan_two = hop2_ids.shape[2]
    share = hidden // devices

    request, groups, held = plan(hop1_ids, hop2_ids, features, devices, row_bits)
    asked = exchange(request.reshape(devices, 1, SLOTS), GX_GY).reshape(devices, SLOTS)
    served = serve(asked, held).reshape(devices, -1, 2, LANES)
    rows = exchange(served, GX_GY).reshape(-1, LANES)

    order = np.arange(hidden, dtype=np.int32).reshape(*sizes, share)
    order = jnp.asarray(np.transpose(order, (3, 0, 2, 1, 4)).reshape(split_c, hidden // split_c))
    core = lax.axis_index("gy_2")
    unit = lax.broadcasted_iota(jnp.int32, (hidden, hidden // split_c), 0)
    hit = unit == lax.dynamic_index_in_dim(order, core, 0)
    turn = hit.astype(BF16)
    turn_other = (unit == lax.dynamic_index_in_dim(order, 1 - core, 0)).astype(BF16)
    self_turned = dot(w_self, turn).astype(BF16)
    neigh_turned = dot(w_neigh, turn).astype(BF16)
    bias_turned = jnp.sum(jnp.where(hit, bias[:, None], 0.0), axis=0)[None, :]
    spread = (cotangent.astype(F32) / (1 + fan_one)).astype(BF16)
    spread_own = dot(spread, turn).astype(BF16)
    spread_pair = dot(swapped(spread), turn).astype(BF16)
    seed_x = features[seed_rows]

    made = (self_turned, neigh_turned, bias_turned, spread_own, spread_pair, seed_x, groups)
    rows, made = lax.optimization_barrier((rows, made))
    *turned, spread_own, spread_pair, seed_x, lanes = made
    own = unpack(rows, lanes, seed_x, fan_one, fan_two)
    pair = swapped(own)
    embedded_own, delta_own = layer(own, *turned, spread_own, fan_one)
    embedded_pair, grad = layer(pair, *turned, spread_pair, fan_one, (own, delta_own))
    embedded = (dot(embedded_own, turn, NT) + dot(swapped(embedded_pair), turn_other, NT)).astype(BF16)

    pieces = exchange(grad.reshape(split_x * split_y, -1, grad.shape[-1]), ("gx", "gy_1"))
    grad = exchange(sum_pieces(pieces, split_z), ("gy_0",)).astype(F32).sum(axis=0)
    return (embedded, grad[:, :width].T, grad[:, width : 2 * width].T, grad[:, 2 * width])


def solution(mesh):
    split = Mesh(mesh.devices.reshape(mesh.shape["gx"], 8, 4, 2), GX_GY)
    rows = P(GX_GY, None)
    in_specs = (rows, P(GX_GY), rows, P(GX_GY, None, None), P(), P(), P(), rows)
    out_specs = (rows, P(None, GX_GY), P(None, GX_GY), P(GX_GY))
    return jax.shard_map(body, mesh=split, in_specs=in_specs, out_specs=out_specs, check_vma=False)
```

```python
import functools

import jax
import jax.numpy as jnp
import numpy as np
from jax import lax
from jax.experimental import pallas as pl
from jax.experimental.pallas import tpu as pltpu
from jax.sharding import Mesh
from jax.sharding import PartitionSpec as P

GX_GY = ("gx", "gy_0", "gy_1", "gy_2")
FAR_CAP = 9
NEAR_CAP = 2
SLOTS = 16
USED = FAR_CAP + NEAR_CAP
LANES = 128
CHUNKS = 4
HALVES = 2
PARTS = 4
SERVED = 4
PLAN_BLOCK = 256
BF16 = jnp.bfloat16
F32 = jnp.float32
INTERPRET = False
KERNEL_VMEM = 40 << 20

NN = (((1,), (0,)), ((), ()))
NT = (((1,), (1,)), ((), ()))


def dot(left, right, dims=NN):
    return lax.dot_general(left, right, dims, preferred_element_type=F32)


ON_CHIP = pl.BlockSpec(memory_space=pltpu.VMEM)


def on_chip(x):
    return pltpu.with_memory_space_constraint(x, pltpu.VMEM)


def plan_kernel(
    devices, row_bits, far_hbm, near_hbm, features_hbm, request_ref, groups_ref, held_ref, far_ref, near_ref, arrived
):
    pairs = ((far_hbm, far_ref), (near_hbm, near_ref), (features_hbm, held_ref))
    copies = [pltpu.make_async_copy(*pair, arrived.at[at]) for at, pair in enumerate(pairs)]
    for copy in copies:
        copy.start()
    for copy in copies[:2]:
        copy.wait()
    fan_one, fan_two, seeds = far_ref.shape
    block = PLAN_BLOCK
    upper = (
        lax.broadcasted_iota(jnp.int32, (block, block), 0) < lax.broadcasted_iota(jnp.int32, (block, block), 1)
    ).astype(F32).astype(BF16)
    owner_at = lax.broadcasted_iota(jnp.int32, (devices, block), 0)
    slot_at = lax.broadcasted_iota(jnp.int32, (SLOTS, block), 0)
    lane = lax.broadcasted_iota(jnp.int32, (1, block), 1)
    found = jnp.zeros((4 * SLOTS, devices), F32)
    far = [(k, far_ref[k, j : j + 1, :]) for k in range(fan_one) for j in range(fan_two)]
    near = [(k, near_ref[k : k + 1, :]) for k in range(fan_one)]
    for first, pieces in ((0, far), (FAR_CAP, near)):
        carry = jnp.zeros((devices, 1), F32)
        for at in range(0, len(pieces), block // seeds):
            here = pieces[at : at + block // seeds]
            rest = block // seeds - len(here)
            ids = jnp.concatenate([ids for _, ids in here] + [jnp.full((1, seeds), -1, jnp.int32)] * rest, axis=1)
            group = lane % seeds + 1
            for place, (k, _) in enumerate(here):
                group = group + jnp.where(lane // seeds == place, k * seeds, 0)
            match = (owner_at == lax.shift_right_arithmetic(ids, row_bits)).astype(F32)
            match_low = match.astype(BF16)
            before = dot(match_low, upper) + carry
            carry = carry + jnp.sum(match, axis=1, keepdims=True)
            rank = jnp.sum(match * before, axis=0, keepdims=True)
            placed = (slot_at == rank.astype(jnp.int32) + first).astype(F32)
            local = ids & ((1 << row_bits) - 1)
            low = local & 31
            group_low = group & 31
            values = (local - low, low, group - group_low, group_low)
            stacked = jnp.concatenate([placed * value.astype(F32) for value in values], axis=0).astype(BF16)
            found = found + dot(stacked, match_low, NT)
    request = found[:SLOTS] + found[SLOTS : 2 * SLOTS]
    groups = found[2 * SLOTS : 3 * SLOTS] + found[3 * SLOTS :]
    request_ref[...] = request.T.astype(jnp.int32)
    groups_ref[...] = groups.astype(jnp.int32) - 1
    copies[2].wait()


def plan(near_ids, far_ids, features, devices, row_bits):
    out = (
        jax.ShapeDtypeStruct((devices, SLOTS), jnp.int32),
        jax.ShapeDtypeStruct((SLOTS, devices), jnp.int32),
        pltpu.VMEM(features.shape, features.dtype),
    )
    far_ids, near_ids = jnp.transpose(far_ids, (1, 2, 0)), jnp.transpose(near_ids)
    inputs = [pltpu.with_memory_space_constraint(x, pltpu.HBM) for x in (far_ids, near_ids, features)]
    return pl.pallas_call(
        functools.partial(plan_kernel, devices, row_bits),
        in_specs=[pl.BlockSpec(memory_space=pltpu.HBM)] * 3,
        out_specs=(ON_CHIP,) * 3,
        out_shape=out,
        scratch_shapes=[
            pltpu.VMEM(far_ids.shape, jnp.int32),
            pltpu.VMEM(near_ids.shape, jnp.int32),
            pltpu.SemaphoreType.DMA((3,)),
        ],
        compiler_params=pltpu.CompilerParams(vmem_limit_bytes=KERNEL_VMEM),
        name="plan",
        interpret=INTERPRET,
    )(*inputs)


def serve_kernel(asked_ref, features_ref, out_hbm, spread_out, out_ref, left):
    rows_dev, width = features_ref.shape
    pieces = width // LANES
    stride = USED * pieces
    peers = asked_ref.shape[0] // SERVED
    lane = lax.broadcasted_iota(jnp.int32, (peers, SLOTS), 1)
    row_at = lax.broadcasted_iota(jnp.int32, (peers, rows_dev), 1).astype(F32)
    copies = []
    for part in range(SERVED):
        asked = asked_ref[part * peers : (part + 1) * peers].astype(F32)
        picks = []
        for slot in range(USED):
            chosen = jnp.sum(jnp.where(lane == slot, asked, 0.0), axis=1, keepdims=True)
            picks.append((row_at == chosen).astype(F32).astype(BF16))
        found = dot(jnp.concatenate(picks, axis=0), features_ref[...])
        first = part * peers * stride
        for slot in range(USED):
            rows = found[slot * peers : (slot + 1) * peers]
            for piece in range(pieces):
                at = first + slot * pieces + piece
                spread_out[pl.ds(at, peers, stride=stride), :] = rows[:, piece * LANES : (piece + 1) * LANES]
        here = pl.ds(first, peers * stride)
        out_ref[here, :] = spread_out[here, :].astype(BF16)
        copies.append(pltpu.make_async_copy(out_ref.at[here], out_hbm.at[here], left.at[part]))
        copies[-1].start()
    for copy in copies:
        copy.wait()


def serve(asked, features):
    devices = asked.shape[0]
    shape = (devices * USED * features.shape[1] // LANES, LANES)
    return pl.pallas_call(
        serve_kernel,
        in_specs=[ON_CHIP, ON_CHIP],
        out_specs=pl.BlockSpec(memory_space=pltpu.HBM),
        out_shape=pltpu.HBM(shape, BF16),
        scratch_shapes=[pltpu.VMEM(shape, F32), pltpu.VMEM(shape, BF16), pltpu.SemaphoreType.DMA((SERVED,))],
        compiler_params=pltpu.CompilerParams(vmem_limit_bytes=KERNEL_VMEM),
        name="serve",
        interpret=INTERPRET,
    )(on_chip(asked), on_chip(features))


def unpack_kernel(fan_one, fan_two, rows_hbm, groups_ref, seed_ref, out_ref, rows_ref, wide, far_acc, near_acc, arrived):
    seeds, width = seed_ref.shape
    pieces = width // LANES
    stride = USED * pieces
    near_total = near_acc.shape[0]
    peers = groups_ref.shape[1]
    share = rows_ref.shape[0] // CHUNKS
    chunks = [pl.ds(at * share, share) for at in range(CHUNKS)]
    copies = [
        pltpu.make_async_copy(rows_hbm.at[here], rows_ref.at[here], arrived.at[at]) for at, here in enumerate(chunks)
    ]
    for copy in copies:
        copy.start()
    half = peers // HALVES
    group_at = lax.broadcasted_iota(jnp.int32, (near_total, half), 0)
    for part in range(HALVES):
        for at in range(part * CHUNKS // HALVES, (part + 1) * CHUNKS // HALVES):
            copies[at].wait()
            wide[chunks[at], :] = rows_ref[chunks[at], :].astype(F32)
        for slots, acc in ((range(FAR_CAP), far_acc), (range(FAR_CAP, USED), near_acc)):
            picks, rows = [], []
            for slot in slots:
                groups = groups_ref[slot : slot + 1, part * half : (part + 1) * half]
                picks.append((group_at == groups).astype(F32).astype(BF16))
                first = part * half * stride + slot * pieces
                at = [wide[pl.ds(first + piece, half, stride=stride), :] for piece in range(pieces)]
                rows.append(jnp.concatenate(at, axis=1).astype(BF16))
            taken = dot(jnp.concatenate(picks, axis=1), jnp.concatenate(rows, axis=0))
            acc[...] = taken if part == 0 else acc[...] + taken
    out_ref[:near_total, :width] = near_acc[...].astype(BF16)
    out_ref[near_total:, :width] = seed_ref[...]
    out_ref[:near_total, width:] = (far_acc[...] / fan_two).astype(BF16)
    summed = near_acc[:seeds]
    for k in range(1, fan_one):
        summed = summed + near_acc[k * seeds : (k + 1) * seeds]
    out_ref[near_total:, width:] = (summed / fan_one).astype(BF16)


def unpack(rows, groups, seed_x, fan_one, fan_two):
    seeds, width = seed_x.shape
    near_total = seeds * fan_one
    return pl.pallas_call(
        functools.partial(unpack_kernel, fan_one, fan_two),
        in_specs=[pl.BlockSpec(memory_space=pltpu.HBM), ON_CHIP, ON_CHIP],
        out_specs=ON_CHIP,
        out_shape=pltpu.VMEM((near_total + seeds, 2 * width), BF16),
        scratch_shapes=[
            pltpu.VMEM(rows.shape, BF16),
            pltpu.VMEM(rows.shape, F32),
            pltpu.VMEM((near_total, width), F32),
            pltpu.VMEM((near_total, width), F32),
            pltpu.SemaphoreType.DMA((CHUNKS,)),
        ],
        compiler_params=pltpu.CompilerParams(vmem_limit_bytes=KERNEL_VMEM),
        name="unpack",
        interpret=INTERPRET,
    )(pltpu.with_memory_space_constraint(rows, pltpu.HBM), on_chip(groups), on_chip(seed_x))


def forward(fan_one, rows_ref, self_ref, neigh_ref, bias_ref, spread_ref, embedded_ref):
    seeds = spread_ref.shape[0]
    width = self_ref.shape[0]
    near_total = seeds * fan_one
    pre = dot(rows_ref[:, :width], self_ref[...]) + dot(rows_ref[:, width:], neigh_ref[...]) + bias_ref[...]
    hidden = jnp.maximum(pre, 0.0).astype(BF16).astype(F32)
    summed = hidden[near_total:]
    for k in range(fan_one):
        summed = summed + hidden[k * seeds : (k + 1) * seeds]
    embedded_ref[...] = (summed / (1 + fan_one)).astype(BF16)
    spread = spread_ref[...].astype(F32)
    return jnp.where(pre > 0, jnp.concatenate([spread] * (1 + fan_one), axis=0), 0.0).T


def first_kernel(fan_one, rows_ref, self_ref, neigh_ref, bias_ref, spread_ref, embedded_ref, turned_ref):
    turned = forward(fan_one, rows_ref, self_ref, neigh_ref, bias_ref, spread_ref, embedded_ref)
    turned_ref[...] = turned.astype(BF16)


def second_kernel(
    fan_one, rows_ref, self_ref, neigh_ref, bias_ref, spread_ref, own_ref, own_turned_ref, embedded_ref, grad_hbm,
    both, turned, grad_ref, left,
):
    count, columns = own_ref.shape
    both[:count] = own_ref[...]
    both[count:] = rows_ref[...]
    turned[:, :count] = own_turned_ref[...]
    pair = forward(fan_one, rows_ref, self_ref, neigh_ref, bias_ref, spread_ref, embedded_ref)
    turned[:, count:] = pair.astype(BF16)
    part = turned.shape[0] // PARTS
    copies = []
    for at in range(PARTS):
        here = pl.ds(at * part, part)
        grad_ref[here, :columns] = dot(turned[here, :], both[...]).astype(BF16)
        summed = jnp.sum(turned[here, :].astype(F32), axis=1, keepdims=True)
        grad_ref[here, columns:] = jnp.broadcast_to(summed, (part, LANES)).astype(BF16)
        copies.append(pltpu.make_async_copy(grad_ref.at[here], grad_hbm.at[here], left.at[at]))
        copies[-1].start()
    for copy in copies:
        copy.wait()


def layer(rows, w_self, w_neigh, bias, spread, fan_one, own=()):
    count, both = rows.shape
    hidden = w_self.shape[1]
    seeds = spread.shape[0]
    inputs = (rows, w_self, w_neigh, bias, spread, *own)
    grads = (hidden, both + LANES)
    scratch = [
        pltpu.VMEM((2 * count, both), BF16),
        pltpu.VMEM((hidden, 2 * count), BF16),
        pltpu.VMEM(grads, BF16),
        pltpu.SemaphoreType.DMA((PARTS,)),
    ]
    return pl.pallas_call(
        functools.partial(second_kernel if own else first_kernel, fan_one),
        in_specs=[ON_CHIP] * len(inputs),
        out_specs=(ON_CHIP, pl.BlockSpec(memory_space=pltpu.HBM) if own else ON_CHIP),
        out_shape=(pltpu.VMEM((seeds, hidden), BF16), pltpu.HBM(grads, BF16) if own else pltpu.VMEM((hidden, count), BF16)),
        scratch_shapes=scratch if own else [],
        compiler_params=pltpu.CompilerParams(vmem_limit_bytes=KERNEL_VMEM),
        name="layer_second" if own else "layer_first",
        interpret=INTERPRET,
    )(*[on_chip(x) for x in inputs])


def sum_kernel(pieces_ref, out_ref):
    summed = pieces_ref[0].astype(F32)
    for at in range(1, pieces_ref.shape[0]):
        summed = summed + pieces_ref[at].astype(F32)
    out_ref[...] = summed.reshape(out_ref.shape).astype(BF16)


def sum_pieces(pieces, groups):
    _, rows, columns = pieces.shape
    return pl.pallas_call(
        sum_kernel,
        in_specs=[ON_CHIP],
        out_specs=ON_CHIP,
        out_shape=pltpu.VMEM((groups, rows // groups, columns), BF16),
        compiler_params=pltpu.CompilerParams(vmem_limit_bytes=KERNEL_VMEM),
        name="sum_pieces",
        interpret=INTERPRET,
    )(on_chip(pieces))


def exchange(pieces, axes):
    return lax.all_to_all(pieces, axes, split_axis=0, concat_axis=0, tiled=True)


def swapped(x):
    return lax.ppermute(x, "gy_2", [(0, 1), (1, 0)])


def body(features, seed_rows, hop1_ids, hop2_ids, w_self, w_neigh, bias, cotangent):
    sizes = [lax.axis_size(a) for a in GX_GY]
    split_x, split_z, split_y, split_c = sizes
    devices = split_x * split_z * split_y * split_c
    rows_dev, width = features.shape
    row_bits = rows_dev.bit_length() - 1
    hidden = w_self.shape[1]
    seeds, fan_one = hop1_ids.shape
    fan_two = hop2_ids.shape[2]
    share = hidden // devices

    request, groups, held = plan(hop1_ids, hop2_ids, features, devices, row_bits)
    asked = exchange(request.reshape(devices, 1, SLOTS), GX_GY).reshape(devices, SLOTS)
    served = serve(asked, held).reshape(devices, -1, 2, LANES)
    rows = exchange(served, GX_GY).reshape(-1, LANES)

    order = np.arange(hidden, dtype=np.int32).reshape(*sizes, share)
    order = jnp.asarray(np.transpose(order, (3, 0, 2, 1, 4)).reshape(split_c, hidden // split_c))
    core = lax.axis_index("gy_2")
    unit = lax.broadcasted_iota(jnp.int32, (hidden, hidden // split_c), 0)
    hit = unit == lax.dynamic_index_in_dim(order, core, 0)
    turn = hit.astype(BF16)
    turn_other = (unit == lax.dynamic_index_in_dim(order, 1 - core, 0)).astype(BF16)
    self_turned = dot(w_self, turn).astype(BF16)
    neigh_turned = dot(w_neigh, turn).astype(BF16)
    bias_turned = jnp.sum(jnp.where(hit, bias[:, None], 0.0), axis=0)[None, :]
    spread = (cotangent.astype(F32) / (1 + fan_one)).astype(BF16)
    spread_own = dot(spread, turn).astype(BF16)
    spread_pair = dot(swapped(spread), turn).astype(BF16)
    seed_x = features[seed_rows]

    made = (self_turned, neigh_turned, bias_turned, spread_own, spread_pair, seed_x, groups)
    rows, made = lax.optimization_barrier((rows, made))
    *turned, spread_own, spread_pair, seed_x, lanes = made
    own = unpack(rows, lanes, seed_x, fan_one, fan_two)
    pair = swapped(own)
    embedded_own, delta_own = layer(own, *turned, spread_own, fan_one)
    embedded_pair, grad = layer(pair, *turned, spread_pair, fan_one, (own, delta_own))
    embedded = (dot(embedded_own, turn, NT) + dot(swapped(embedded_pair), turn_other, NT)).astype(BF16)

    pieces = exchange(grad.reshape(split_x * split_y, -1, grad.shape[-1]), ("gx", "gy_1"))
    grad = exchange(sum_pieces(pieces, split_z), ("gy_0",)).astype(F32).sum(axis=0)
    return (embedded, grad[:, :width].T, grad[:, width : 2 * width].T, grad[:, 2 * width])


def solution(mesh):
    split = Mesh(mesh.devices.reshape(mesh.shape["gx"], 8, 4, 2), GX_GY)
    rows = P(GX_GY, None)
    in_specs = (rows, P(GX_GY), rows, P(GX_GY, None, None), P(), P(), P(), rows)
    out_specs = (rows, P(None, GX_GY), P(None, GX_GY), P(GX_GY))
    return jax.shard_map(body, mesh=split, in_specs=in_specs, out_specs=out_specs, check_vma=False)
```

```python
import functools

import jax
import jax.numpy as jnp
import numpy as np
from jax import lax
from jax.experimental import pallas as pl
from jax.experimental.pallas import tpu as pltpu
from jax.sharding import Mesh
from jax.sharding import PartitionSpec as P

GX_GY = ("gx", "gy_0", "gy_1", "gy_2")
FAR_CAP = 9
NEAR_CAP = 2
SLOTS = 16
USED = FAR_CAP + NEAR_CAP
LANES = 128
CHUNKS = 4
HALVES = 2
PARTS = 4
SERVED = 8
PLAN_BLOCK = 256
BF16 = jnp.bfloat16
F32 = jnp.float32
INTERPRET = False
KERNEL_VMEM = 40 << 20

NN = (((1,), (0,)), ((), ()))
NT = (((1,), (1,)), ((), ()))


def dot(left, right, dims=NN):
    return lax.dot_general(left, right, dims, preferred_element_type=F32)


ON_CHIP = pl.BlockSpec(memory_space=pltpu.VMEM)


def on_chip(x):
    return pltpu.with_memory_space_constraint(x, pltpu.VMEM)


def plan_kernel(
    devices, row_bits, far_hbm, near_hbm, features_hbm, request_ref, groups_ref, held_ref, far_ref, near_ref, arrived
):
    pairs = ((far_hbm, far_ref), (near_hbm, near_ref), (features_hbm, held_ref))
    copies = [pltpu.make_async_copy(*pair, arrived.at[at]) for at, pair in enumerate(pairs)]
    for copy in copies:
        copy.start()
    for copy in copies[:2]:
        copy.wait()
    fan_one, fan_two, seeds = far_ref.shape
    block = PLAN_BLOCK
    upper = (
        lax.broadcasted_iota(jnp.int32, (block, block), 0) < lax.broadcasted_iota(jnp.int32, (block, block), 1)
    ).astype(F32).astype(BF16)
    owner_at = lax.broadcasted_iota(jnp.int32, (devices, block), 0)
    slot_at = lax.broadcasted_iota(jnp.int32, (SLOTS, block), 0)
    lane = lax.broadcasted_iota(jnp.int32, (1, block), 1)
    found = jnp.zeros((4 * SLOTS, devices), F32)
    far = [(k, far_ref[k, j : j + 1, :]) for k in range(fan_one) for j in range(fan_two)]
    near = [(k, near_ref[k : k + 1, :]) for k in range(fan_one)]
    for first, pieces in ((0, far), (FAR_CAP, near)):
        carry = jnp.zeros((devices, 1), F32)
        for at in range(0, len(pieces), block // seeds):
            here = pieces[at : at + block // seeds]
            rest = block // seeds - len(here)
            ids = jnp.concatenate([ids for _, ids in here] + [jnp.full((1, seeds), -1, jnp.int32)] * rest, axis=1)
            group = lane % seeds + 1
            for place, (k, _) in enumerate(here):
                group = group + jnp.where(lane // seeds == place, k * seeds, 0)
            match = (owner_at == lax.shift_right_arithmetic(ids, row_bits)).astype(F32)
            match_low = match.astype(BF16)
            before = dot(match_low, upper) + carry
            carry = carry + jnp.sum(match, axis=1, keepdims=True)
            rank = jnp.sum(match * before, axis=0, keepdims=True)
            placed = (slot_at == rank.astype(jnp.int32) + first).astype(F32)
            local = ids & ((1 << row_bits) - 1)
            low = local & 31
            group_low = group & 31
            values = (local - low, low, group - group_low, group_low)
            stacked = jnp.concatenate([placed * value.astype(F32) for value in values], axis=0).astype(BF16)
            found = found + dot(stacked, match_low, NT)
    request = found[:SLOTS] + found[SLOTS : 2 * SLOTS]
    groups = found[2 * SLOTS : 3 * SLOTS] + found[3 * SLOTS :]
    request_ref[...] = request.T.astype(jnp.int32)
    groups_ref[...] = groups.astype(jnp.int32) - 1
    copies[2].wait()


def plan(near_ids, far_ids, features, devices, row_bits):
    out = (
        jax.ShapeDtypeStruct((devices, SLOTS), jnp.int32),
        jax.ShapeDtypeStruct((SLOTS, devices), jnp.int32),
        pltpu.VMEM(features.shape, features.dtype),
    )
    far_ids, near_ids = jnp.transpose(far_ids, (1, 2, 0)), jnp.transpose(near_ids)
    inputs = [pltpu.with_memory_space_constraint(x, pltpu.HBM) for x in (far_ids, near_ids, features)]
    return pl.pallas_call(
        functools.partial(plan_kernel, devices, row_bits),
        in_specs=[pl.BlockSpec(memory_space=pltpu.HBM)] * 3,
        out_specs=(ON_CHIP,) * 3,
        out_shape=out,
        scratch_shapes=[
            pltpu.VMEM(far_ids.shape, jnp.int32),
            pltpu.VMEM(near_ids.shape, jnp.int32),
            pltpu.SemaphoreType.DMA((3,)),
        ],
        compiler_params=pltpu.CompilerParams(vmem_limit_bytes=KERNEL_VMEM),
        name="plan",
        interpret=INTERPRET,
    )(*inputs)


def serve_kernel(asked_ref, features_ref, out_hbm, spread_out, out_ref, left):
    rows_dev, width = features_ref.shape
    pieces = width // LANES
    stride = USED * pieces
    peers = asked_ref.shape[0] // SERVED
    lane = lax.broadcasted_iota(jnp.int32, (peers, SLOTS), 1)
    row_at = lax.broadcasted_iota(jnp.int32, (peers, rows_dev), 1).astype(F32)
    copies = []
    for part in range(SERVED):
        asked = asked_ref[part * peers : (part + 1) * peers].astype(F32)
        picks = []
        for slot in range(USED):
            chosen = jnp.sum(jnp.where(lane == slot, asked, 0.0), axis=1, keepdims=True)
            picks.append((row_at == chosen).astype(F32).astype(BF16))
        found = dot(jnp.concatenate(picks, axis=0), features_ref[...])
        first = part * peers * stride
        for slot in range(USED):
            rows = found[slot * peers : (slot + 1) * peers]
            for piece in range(pieces):
                at = first + slot * pieces + piece
                spread_out[pl.ds(at, peers, stride=stride), :] = rows[:, piece * LANES : (piece + 1) * LANES]
        here = pl.ds(first, peers * stride)
        out_ref[here, :] = spread_out[here, :].astype(BF16)
        copies.append(pltpu.make_async_copy(out_ref.at[here], out_hbm.at[here], left.at[part]))
        copies[-1].start()
    for copy in copies:
        copy.wait()


def serve(asked, features):
    devices = asked.shape[0]
    shape = (devices * USED * features.shape[1] // LANES, LANES)
    return pl.pallas_call(
        serve_kernel,
        in_specs=[ON_CHIP, ON_CHIP],
        out_specs=pl.BlockSpec(memory_space=pltpu.HBM),
        out_shape=pltpu.HBM(shape, BF16),
        scratch_shapes=[pltpu.VMEM(shape, F32), pltpu.VMEM(shape, BF16), pltpu.SemaphoreType.DMA((SERVED,))],
        compiler_params=pltpu.CompilerParams(vmem_limit_bytes=KERNEL_VMEM),
        name="serve",
        interpret=INTERPRET,
    )(on_chip(asked), on_chip(features))


def unpack_kernel(fan_one, fan_two, rows_hbm, groups_ref, seed_ref, out_ref, rows_ref, wide, far_acc, near_acc, arrived):
    seeds, width = seed_ref.shape
    pieces = width // LANES
    stride = USED * pieces
    near_total = near_acc.shape[0]
    peers = groups_ref.shape[1]
    share = rows_ref.shape[0] // CHUNKS
    chunks = [pl.ds(at * share, share) for at in range(CHUNKS)]
    copies = [
        pltpu.make_async_copy(rows_hbm.at[here], rows_ref.at[here], arrived.at[at]) for at, here in enumerate(chunks)
    ]
    for copy in copies:
        copy.start()
    half = peers // HALVES
    group_at = lax.broadcasted_iota(jnp.int32, (near_total, half), 0)
    for part in range(HALVES):
        for at in range(part * CHUNKS // HALVES, (part + 1) * CHUNKS // HALVES):
            copies[at].wait()
            wide[chunks[at], :] = rows_ref[chunks[at], :].astype(F32)
        for slots, acc in ((range(FAR_CAP), far_acc), (range(FAR_CAP, USED), near_acc)):
            picks, rows = [], []
            for slot in slots:
                groups = groups_ref[slot : slot + 1, part * half : (part + 1) * half]
                picks.append((group_at == groups).astype(F32).astype(BF16))
                first = part * half * stride + slot * pieces
                at = [wide[pl.ds(first + piece, half, stride=stride), :] for piece in range(pieces)]
                rows.append(jnp.concatenate(at, axis=1).astype(BF16))
            taken = dot(jnp.concatenate(picks, axis=1), jnp.concatenate(rows, axis=0))
            acc[...] = taken if part == 0 else acc[...] + taken
    out_ref[:near_total, :width] = near_acc[...].astype(BF16)
    out_ref[near_total:, :width] = seed_ref[...]
    out_ref[:near_total, width:] = (far_acc[...] / fan_two).astype(BF16)
    summed = near_acc[:seeds]
    for k in range(1, fan_one):
        summed = summed + near_acc[k * seeds : (k + 1) * seeds]
    out_ref[near_total:, width:] = (summed / fan_one).astype(BF16)


def unpack(rows, groups, seed_x, fan_one, fan_two):
    seeds, width = seed_x.shape
    near_total = seeds * fan_one
    return pl.pallas_call(
        functools.partial(unpack_kernel, fan_one, fan_two),
        in_specs=[pl.BlockSpec(memory_space=pltpu.HBM), ON_CHIP, ON_CHIP],
        out_specs=ON_CHIP,
        out_shape=pltpu.VMEM((near_total + seeds, 2 * width), BF16),
        scratch_shapes=[
            pltpu.VMEM(rows.shape, BF16),
            pltpu.VMEM(rows.shape, F32),
            pltpu.VMEM((near_total, width), F32),
            pltpu.VMEM((near_total, width), F32),
            pltpu.SemaphoreType.DMA((CHUNKS,)),
        ],
        compiler_params=pltpu.CompilerParams(vmem_limit_bytes=KERNEL_VMEM),
        name="unpack",
        interpret=INTERPRET,
    )(pltpu.with_memory_space_constraint(rows, pltpu.HBM), on_chip(groups), on_chip(seed_x))


def forward(fan_one, rows_ref, self_ref, neigh_ref, bias_ref, spread_ref, embedded_ref):
    seeds = spread_ref.shape[0]
    width = self_ref.shape[0]
    near_total = seeds * fan_one
    pre = dot(rows_ref[:, :width], self_ref[...]) + dot(rows_ref[:, width:], neigh_ref[...]) + bias_ref[...]
    hidden = jnp.maximum(pre, 0.0).astype(BF16).astype(F32)
    summed = hidden[near_total:]
    for k in range(fan_one):
        summed = summed + hidden[k * seeds : (k + 1) * seeds]
    embedded_ref[...] = (summed / (1 + fan_one)).astype(BF16)
    spread = spread_ref[...].astype(F32)
    return jnp.where(pre > 0, jnp.concatenate([spread] * (1 + fan_one), axis=0), 0.0).T


def first_kernel(fan_one, rows_ref, self_ref, neigh_ref, bias_ref, spread_ref, embedded_ref, turned_ref):
    turned = forward(fan_one, rows_ref, self_ref, neigh_ref, bias_ref, spread_ref, embedded_ref)
    turned_ref[...] = turned.astype(BF16)


def second_kernel(
    fan_one, rows_ref, self_ref, neigh_ref, bias_ref, spread_ref, own_ref, own_turned_ref, embedded_ref, grad_hbm,
    both, turned, grad_ref, left,
):
    count, columns = own_ref.shape
    both[:count] = own_ref[...]
    both[count:] = rows_ref[...]
    turned[:, :count] = own_turned_ref[...]
    pair = forward(fan_one, rows_ref, self_ref, neigh_ref, bias_ref, spread_ref, embedded_ref)
    turned[:, count:] = pair.astype(BF16)
    part = turned.shape[0] // PARTS
    copies = []
    for at in range(PARTS):
        here = pl.ds(at * part, part)
        grad_ref[here, :columns] = dot(turned[here, :], both[...]).astype(BF16)
        summed = jnp.sum(turned[here, :].astype(F32), axis=1, keepdims=True)
        grad_ref[here, columns:] = jnp.broadcast_to(summed, (part, LANES)).astype(BF16)
        copies.append(pltpu.make_async_copy(grad_ref.at[here], grad_hbm.at[here], left.at[at]))
        copies[-1].start()
    for copy in copies:
        copy.wait()


def layer(rows, w_self, w_neigh, bias, spread, fan_one, own=()):
    count, both = rows.shape
    hidden = w_self.shape[1]
    seeds = spread.shape[0]
    inputs = (rows, w_self, w_neigh, bias, spread, *own)
    grads = (hidden, both + LANES)
    scratch = [
        pltpu.VMEM((2 * count, both), BF16),
        pltpu.VMEM((hidden, 2 * count), BF16),
        pltpu.VMEM(grads, BF16),
        pltpu.SemaphoreType.DMA((PARTS,)),
    ]
    return pl.pallas_call(
        functools.partial(second_kernel if own else first_kernel, fan_one),
        in_specs=[ON_CHIP] * len(inputs),
        out_specs=(ON_CHIP, pl.BlockSpec(memory_space=pltpu.HBM) if own else ON_CHIP),
        out_shape=(pltpu.VMEM((seeds, hidden), BF16), pltpu.HBM(grads, BF16) if own else pltpu.VMEM((hidden, count), BF16)),
        scratch_shapes=scratch if own else [],
        compiler_params=pltpu.CompilerParams(vmem_limit_bytes=KERNEL_VMEM),
        name="layer_second" if own else "layer_first",
        interpret=INTERPRET,
    )(*[on_chip(x) for x in inputs])


def sum_kernel(pieces_ref, out_ref):
    summed = pieces_ref[0].astype(F32)
    for at in range(1, pieces_ref.shape[0]):
        summed = summed + pieces_ref[at].astype(F32)
    out_ref[...] = summed.reshape(out_ref.shape).astype(BF16)


def sum_pieces(pieces, groups):
    _, rows, columns = pieces.shape
    return pl.pallas_call(
        sum_kernel,
        in_specs=[ON_CHIP],
        out_specs=ON_CHIP,
        out_shape=pltpu.VMEM((groups, rows // groups, columns), BF16),
        compiler_params=pltpu.CompilerParams(vmem_limit_bytes=KERNEL_VMEM),
        name="sum_pieces",
        interpret=INTERPRET,
    )(on_chip(pieces))


def last_kernel(pieces_ref, self_hbm, neigh_hbm, bias_hbm, self_ref, neigh_ref, bias_ref, left):
    share, width = self_ref.shape
    summed = pieces_ref[0].astype(F32)
    for at in range(1, pieces_ref.shape[0]):
        summed = summed + pieces_ref[at].astype(F32)
    self_ref[...] = summed[:, :width]
    neigh_ref[...] = summed[:, width : 2 * width]
    square = (share, share)
    here = lax.broadcasted_iota(jnp.int32, square, 0) == lax.broadcasted_iota(jnp.int32, square, 1)
    column = jnp.broadcast_to(summed[:, 2 * width : 2 * width + 1], square)
    bias_ref[...] = jnp.sum(jnp.where(here, column, 0.0), axis=0, keepdims=True)
    pairs = ((self_ref, self_hbm), (neigh_ref, neigh_hbm), (bias_ref, bias_hbm))
    copies = [pltpu.make_async_copy(*pair, left.at[at]) for at, pair in enumerate(pairs)]
    for copy in copies:
        copy.start()
    for copy in copies:
        copy.wait()


def last(pieces, width):
    share = pieces.shape[1]
    shapes = ((share, width), (share, width), (1, share))
    return pl.pallas_call(
        last_kernel,
        in_specs=[ON_CHIP],
        out_specs=(pl.BlockSpec(memory_space=pltpu.HBM),) * 3,
        out_shape=tuple(pltpu.HBM(shape, F32) for shape in shapes),
        scratch_shapes=[*[pltpu.VMEM(shape, F32) for shape in shapes], pltpu.SemaphoreType.DMA((3,))],
        compiler_params=pltpu.CompilerParams(vmem_limit_bytes=KERNEL_VMEM),
        name="last",
        interpret=INTERPRET,
    )(on_chip(pieces))


def exchange(pieces, axes):
    return lax.all_to_all(pieces, axes, split_axis=0, concat_axis=0, tiled=True)


def swapped(x):
    return lax.ppermute(x, "gy_2", [(0, 1), (1, 0)])


def body(features, seed_rows, hop1_ids, hop2_ids, w_self, w_neigh, bias, cotangent):
    sizes = [lax.axis_size(a) for a in GX_GY]
    split_x, split_z, split_y, split_c = sizes
    devices = split_x * split_z * split_y * split_c
    rows_dev, width = features.shape
    row_bits = rows_dev.bit_length() - 1
    hidden = w_self.shape[1]
    seeds, fan_one = hop1_ids.shape
    fan_two = hop2_ids.shape[2]
    share = hidden // devices

    request, groups, held = plan(hop1_ids, hop2_ids, features, devices, row_bits)
    asked = exchange(request.reshape(devices, 1, SLOTS), GX_GY).reshape(devices, SLOTS)
    served = serve(asked, held).reshape(devices, -1, 2, LANES)
    rows = exchange(served, GX_GY).reshape(-1, LANES)

    order = np.arange(hidden, dtype=np.int32).reshape(*sizes, share)
    order = jnp.asarray(np.transpose(order, (3, 0, 2, 1, 4)).reshape(split_c, hidden // split_c))
    core = lax.axis_index("gy_2")
    unit = lax.broadcasted_iota(jnp.int32, (hidden, hidden // split_c), 0)
    hit = unit == lax.dynamic_index_in_dim(order, core, 0)
    turn = hit.astype(BF16)
    turn_other = (unit == lax.dynamic_index_in_dim(order, 1 - core, 0)).astype(BF16)
    self_turned = dot(w_self, turn).astype(BF16)
    neigh_turned = dot(w_neigh, turn).astype(BF16)
    bias_turned = jnp.sum(jnp.where(hit, bias[:, None], 0.0), axis=0)[None, :]
    spread = (cotangent.astype(F32) / (1 + fan_one)).astype(BF16)
    spread_own = dot(spread, turn).astype(BF16)
    spread_pair = dot(swapped(spread), turn).astype(BF16)
    seed_x = features[seed_rows]

    made = (self_turned, neigh_turned, bias_turned, spread_own, spread_pair, seed_x, groups)
    rows, made = lax.optimization_barrier((rows, made))
    *turned, spread_own, spread_pair, seed_x, lanes = made
    own = unpack(rows, lanes, seed_x, fan_one, fan_two)
    pair = swapped(own)
    embedded_own, delta_own = layer(own, *turned, spread_own, fan_one)
    embedded_pair, grad = layer(pair, *turned, spread_pair, fan_one, (own, delta_own))
    embedded = (dot(embedded_own, turn, NT) + dot(swapped(embedded_pair), turn_other, NT)).astype(BF16)

    pieces = exchange(grad.reshape(split_x * split_y, -1, grad.shape[-1]), ("gx", "gy_1"))
    pieces = exchange(sum_pieces(pieces, split_z), ("gy_0",))
    grad_self, grad_neigh, grad_bias = last(pieces, width)
    return (embedded, grad_self.T, grad_neigh.T, grad_bias.reshape(-1))


def solution(mesh):
    split = Mesh(mesh.devices.reshape(mesh.shape["gx"], 8, 4, 2), GX_GY)
    rows = P(GX_GY, None)
    in_specs = (rows, P(GX_GY), rows, P(GX_GY, None, None), P(), P(), P(), rows)
    out_specs = (rows, P(None, GX_GY), P(None, GX_GY), P(GX_GY))
    return jax.shard_map(body, mesh=split, in_specs=in_specs, out_specs=out_specs, check_vma=False)
```
